128 devices in a mesh: slot: 32 (over x, z, y_hi), dp: 4 (over y_lo, core).
Axes of the slice: x: 4, y: 4 (y_hi: 2, y_lo: 2; y = y_hi * 2 + y_lo), z: 4, core: 2. Of those that a mesh axis runs over, the one named last changes fastest.
Arguments:
- tokens: bfloat16 [12, 4096, 1024], P('dp', 'slot'), may hold values from -6 to 6
- slot_keys: bfloat16 [1024, 1024], P(None, 'slot'), may hold values from -1.5 to 1.5
- expert_in: bfloat16 [128, 1024, 4096], P('slot', None, 'dp'), may hold values from -0.5 to 0.5
- expert_out: bfloat16 [128, 4096, 1024], P('slot', 'dp'), may hold values from -0.1875 to 0.1875
Outputs:
- combined: bfloat16 [12, 4096, 1024], P('dp', 'slot')
The draws below stay inside these ranges and needn't reach their ends.
All inputs are finite; a program needn't handle non-finite values.
Results may differ from the reference program's by a relative error of at most 0.0085.
Values may be sent and summed in bfloat16 or wider, within the bound.
No kernel may reach another device: no remote copies, remote signals or barrier semaphores. Data moves between devices by JAX's collectives and lax.ppermute only.
A program may use at most 128 MiB of HBM per device.

```python
import jax
import jax.numpy as jnp
from jax import lax

D = 1024
FF = 4096
SLOTS_EXP = 8
IMG_TOK = 4096
EXPERTS = 128
SLOTS = 1024
BATCH = 12


def token_field(key):
    values = jax.random.normal(jax.random.fold_in(key, 11), (BATCH, IMG_TOK, D), jnp.float32)
    return jnp.clip(values, -6.0, 6.0)


def draw_tokens(key, part):
    return token_field(key).astype(jnp.bfloat16)


def draw_slot_keys(key, part):
    base = 0.125 * jnp.clip(jax.random.normal(jax.random.fold_in(key, 23), (D, SLOTS), jnp.float32), -6.0, 6.0)
    return base.astype(jnp.bfloat16)


def steps_of(key, extent, cuts, smallest, top_value):
    def one(position, parts):
        steps = jax.random.uniform(jax.random.fold_in(jax.random.fold_in(key, 6), position), (parts,), jnp.float32, smallest / len(cuts), top_value / len(cuts))
        return jnp.repeat(jnp.exp(steps), extent[position] // parts).reshape((-1,) + (1,) * (len(extent) - position - 1))

    gain = one(*cuts[0])
    for cut in cuts[1:]:
        gain = gain * one(*cut)
    return gain


def noise(rng, extent, scale, most, split=(), dtype=jnp.bfloat16):
    result = jax.random.normal(rng, extent, jnp.float32) * scale
    if len(split) > 0:
        result = steps_of(rng, extent, split, -0.22, 0.18) * result
    return jnp.clip(result, min=-most, max=most).astype(dtype)


def setup_inputs(seed: int = 0) -> dict:
    seeds = jax.random.split(jax.random.key(seed), 5)
    tokens = draw_tokens(jax.random.fold_in(seeds[4], 71), 0)
    slot_keys = draw_slot_keys(jax.random.fold_in(seeds[4], 71), 0)
    expert_in = noise(seeds[2], (EXPERTS, D, FF), (D // 8) ** -0.5, 0.5, ((0, 32), (2, 4)))
    expert_out = noise(seeds[3], (EXPERTS, FF, D), (FF // 4) ** -0.5, 0.1875, ((0, 32), (1, 4)))
    return dict(tokens=tokens, slot_keys=slot_keys, expert_in=expert_in, expert_out=expert_out)


def reference(tokens, slot_keys, expert_in, expert_out):
    flat = tokens.reshape(BATCH * IMG_TOK, D)
    logits = jnp.dot(flat, slot_keys, preferred_element_type=jnp.float32).reshape(BATCH, IMG_TOK, SLOTS)
    peak = jnp.max(logits, axis=1, keepdims=True)
    raised = jnp.exp(logits - peak)
    totals = jnp.sum(raised, axis=1)
    weights = raised.astype(jnp.bfloat16)
    gathered = jnp.einsum('bms,bmd->bsd', weights.astype(jnp.float32), tokens.astype(jnp.float32))
    slot_inputs = (gathered / totals[:, :, None]).astype(jnp.bfloat16)
    expert_rows = slot_inputs.reshape(BATCH, EXPERTS, SLOTS_EXP, D).transpose(1, 0, 2, 3)
    expert_rows = expert_rows.reshape(EXPERTS, BATCH * SLOTS_EXP, D)

    def run_expert(operands):
        rows, first, second = operands
        hidden = jax.nn.gelu(jnp.dot(rows, first, preferred_element_type=jnp.float32), approximate=True)
        hidden = hidden.astype(jnp.bfloat16)
        return jnp.dot(hidden, second, preferred_element_type=jnp.float32).astype(jnp.bfloat16)

    outputs = lax.map(run_expert, (expert_rows, expert_in, expert_out))
    slot_outputs = outputs.reshape(EXPERTS, BATCH, SLOTS_EXP, D).transpose(1, 0, 2, 3).reshape(BATCH, SLOTS, D)
    mix = jax.nn.softmax(logits, axis=2).astype(jnp.bfloat16)
    combined = jnp.einsum('bms,bsd->bmd', mix.astype(jnp.float32), slot_outputs.astype(jnp.float32))
    return combined.astype(jnp.bfloat16)
```

```python
import jax
import jax.numpy as jnp
from jax import lax
from jax.sharding import Mesh
from jax.sharding import PartitionSpec as P

X, Z, Y = "slot_0", "slot_1", "slot_2"
SLOT = (X, Z, Y)
COLOURS = ((X, Z), (Z, X))


def ahead(array, axis, step):
    if step == 0:
        return array
    size = lax.axis_size(axis)
    return lax.ppermute(array, axis, [((i + step) % size, i) for i in range(size)])


def onward(array, axis, step):
    if step == 0:
        return array
    size = lax.axis_size(axis)
    return lax.ppermute(array, axis, [(i, (i + step) % size) for i in range(size)])


def swapped(array, axis, mask):
    if mask == 0:
        return array
    size = lax.axis_size(axis)
    return lax.ppermute(array, axis, [(i, i ^ mask) for i in range(size)])


def collected(array, axes, dim):
    for axis in axes:
        steps = range(lax.axis_size(axis))
        array = jnp.concatenate([ahead(array, axis, k) for k in steps], axis=dim)
    return array


def merged(parts):
    sums, tops, totals = zip(*parts)
    top = tops[0]
    for other in tops[1:]:
        top = jnp.maximum(top, other)
    scales = [jnp.exp(t - top) for t in tops]
    total = sum(f * t for f, t in zip(scales, totals))
    joined = sum(f[..., None] * s.astype(jnp.float32) for f, s in zip(scales, sums))
    return joined, top, total


def scattered(sums, top, total, axis):
    size = lax.axis_size(axis)
    rows = top.shape[1] // size
    parts = []
    for k in range(size):
        cut = slice(k * rows, (k + 1) * rows)
        piece = (sums[k] if isinstance(sums, list) else sums[:, cut]).astype(jnp.bfloat16)
        stats = jnp.stack([top[:, cut], total[:, cut]])
        stats = onward(stats, axis, k)
        parts.append((onward(piece, axis, k), stats[0], stats[1]))
    return merged(parts)


def shards(tokens, slot_keys, expert_in, expert_out):
    images, positions, features = tokens.shape
    own_slots = slot_keys.shape[1]
    experts = expert_in.shape[0]
    per_expert = own_slots // experts
    half = own_slots // 2
    keys = slot_keys.T
    field = jnp.concatenate([tokens, ahead(tokens, Y, 1)], axis=1)
    all_logits, inputs = [], []
    for c, axes in enumerate(COLOURS):
        mine = collected(keys[c * half : (c + 1) * half], axes, 0)
        logits = jnp.einsum("sd,bmd->bsm", mine, field, preferred_element_type=jnp.float32)
        top = jnp.max(logits, axis=2)
        raised = jnp.exp(logits - top[:, :, None])
        total = jnp.sum(raised, axis=2)
        weights = raised.astype(jnp.bfloat16)
        size = lax.axis_size(axes[1])
        rows = weights.shape[1] // size
        sums = [
            jnp.einsum(
                "bsm,bmd->bsd",
                weights[:, k * rows : (k + 1) * rows],
                field,
                preferred_element_type=jnp.float32,
            )
            for k in range(size)
        ]
        sums, top, total = scattered(sums, top, total, axes[1])
        sums, top, total = scattered(sums, top, total, axes[0])
        inputs.append((sums / total[:, :, None]).astype(jnp.bfloat16))
        all_logits.append(logits)
    slot_inputs = jnp.concatenate(inputs, axis=1)
    ranks = lax.axis_size("dp")
    rows = jnp.stack([swapped(slot_inputs, "dp", k) for k in range(ranks)])
    rows = rows.reshape(ranks * images, experts, per_expert, features)
    rows = rows.transpose(1, 0, 2, 3).reshape(experts, -1, features)
    hidden = jnp.einsum("erd,edf->erf", rows, expert_in, preferred_element_type=jnp.float32)
    hidden = jax.nn.gelu(hidden, approximate=True).astype(jnp.bfloat16)
    result = jnp.einsum("erf,efd->erd", hidden, expert_out, preferred_element_type=jnp.float32)
    result = result.reshape(experts, ranks, images, per_expert, features)
    result = result.transpose(1, 2, 0, 3, 4).reshape(ranks, images, own_slots, features)
    outputs = result[0]
    for k in range(1, ranks):
        outputs = outputs + swapped(result[k].astype(jnp.bfloat16), "dp", k).astype(jnp.float32)
    outputs = outputs.astype(jnp.bfloat16)
    top = jnp.maximum(jnp.max(all_logits[0], axis=1), jnp.max(all_logits[1], axis=1))
    total = sum(jnp.sum(jnp.exp(l - top[:, None, :]), axis=1) for l in all_logits)
    theirs = ahead(jnp.stack([top, total]), Y, 1)
    theirs = jnp.concatenate([theirs[:, :, positions:], theirs[:, :, :positions]], axis=2)
    highest = jnp.maximum(top, theirs[0])
    total = total * jnp.exp(top - highest) + theirs[1] * jnp.exp(theirs[0] - highest)
    combined = 0.0
    for c, axes in enumerate(COLOURS):
        mix = jnp.exp(all_logits[c] - highest[:, None, :]) / total[:, None, :]
        everyone = collected(outputs[:, c * half : (c + 1) * half], axes, 1)
        combined = combined + jnp.einsum(
            "bsm,bsd->bmd",
            mix.astype(jnp.bfloat16),
            everyone,
            preferred_element_type=jnp.float32,
        )
    away = ahead(combined[:, positions:].astype(jnp.bfloat16), Y, 1)
    return (combined[:, :positions] + away.astype(jnp.float32)).astype(jnp.bfloat16)


def solution(mesh):
    split = Mesh(
        mesh.devices.reshape(4, 4, 2, mesh.shape["dp"]), (X, Z, Y, "dp")
    )
    return jax.shard_map(
        shards,
        mesh=split,
        in_specs=(P("dp", SLOT, None), P(None, SLOT), P(SLOT, None, "dp"), P(SLOT, "dp", None)),
        out_specs=P("dp", SLOT, None),
        check_vma=False,
    )
```

```python
import jax
import jax.numpy as jnp
from jax import lax
from jax.sharding import Mesh
from jax.sharding import PartitionSpec as P

X, Z, Y = "slot_0", "slot_1", "slot_2"
SLOT = (X, Z, Y)
OWNERS = (Z, Y)
STAT_ROWS = 8


def ahead(array, axis, step):
    size = lax.axis_size(axis)
    return lax.ppermute(array, axis, [((i + step) % size, i) for i in range(size)])


def swapped(array, axis, mask):
    size = lax.axis_size(axis)
    return lax.ppermute(array, axis, [(i, i ^ mask) for i in range(size)])


def to_everyone(array, axis):
    copies = jnp.broadcast_to(array, (lax.axis_size(axis), *array.shape))
    return lax.all_to_all(copies, axis, split_axis=0, concat_axis=0, tiled=True)


def bf16_pieces(value, count):
    pieces = []
    for _ in range(count):
        piece = lax.reduce_precision(value, 8, 7)
        pieces.append(piece)
        value = value - piece
    return pieces


def shards(tokens, slot_keys, expert_in, expert_out):
    images, positions, features = tokens.shape
    own_slots = slot_keys.shape[1]
    experts = expert_in.shape[0]
    per_expert = own_slots // experts
    owners = lax.axis_size(OWNERS)
    ranks = lax.axis_size("dp")
    mid = positions // 2

    right = ahead(tokens, X, 1)
    left = ahead(tokens, X, 3)
    keys = to_everyone(slot_keys.T, OWNERS).reshape(owners * own_slots, features)
    far_low = ahead(right[:, :mid], X, 1)
    far_high = ahead(left[:, mid:], X, 3)
    field = jnp.concatenate([tokens, right, far_low, far_high, left], axis=1)

    logits = jnp.einsum("sd,bmd->bsm", keys, field, preferred_element_type=jnp.float32)
    top = lax.reduce_precision(jnp.max(logits, axis=2), 8, 7)
    raised = jnp.exp(logits - top[:, :, None])
    total = jnp.sum(raised, axis=2)
    sums = jnp.einsum(
        "bsm,bmd->bsd", raised.astype(jnp.bfloat16), field, preferred_element_type=jnp.float32
    ).astype(jnp.bfloat16)
    stats = jnp.stack([top, *bf16_pieces(total, 3)]).astype(jnp.bfloat16)
    count = stats.shape[0] * images * own_slots
    stats = stats.reshape(-1, images, owners, own_slots).transpose(2, 0, 1, 3).reshape(owners, count)
    stats = jnp.pad(stats, ((0, 0), (0, STAT_ROWS * features - count)))
    sums = sums.reshape(images, owners, own_slots, features).transpose(1, 0, 2, 3)
    message = jnp.concatenate(
        [
            sums.reshape(owners, images * own_slots, features),
            stats.reshape(owners, STAT_ROWS, features),
        ],
        axis=1,
    )
    arrived = lax.all_to_all(message, OWNERS, split_axis=0, concat_axis=0, tiled=True)

    row_top = jnp.max(logits, axis=1)
    row_total = jnp.sum(jnp.exp(logits - row_top[:, None, :]), axis=1)
    row_stats = jnp.stack([row_top, row_total])
    others = [ahead(row_stats, X, k) for k in (1, 2, 3)]
    others = [jnp.roll(o, k * positions, axis=2) for k, o in zip((1, 2, 3), others)]
    highest = row_top
    for o in others:
        highest = jnp.maximum(highest, o[0])
    whole = row_total * jnp.exp(row_top - highest)
    for o in others:
        whole = whole + o[1] * jnp.exp(o[0] - highest)
    mix = (jnp.exp(logits - highest[:, None, :]) / whole[:, None, :]).astype(jnp.bfloat16)

    cut = images * own_slots
    stats = arrived[:, cut:].reshape(owners, -1)[:, :count].astype(jnp.float32)
    stats = stats.reshape(owners, -1, images * own_slots)
    peak = jnp.max(stats[:, 0], axis=0)
    scale = jnp.exp(stats[:, 0] - peak)
    share = scale / jnp.sum(scale * (stats[:, 1] + stats[:, 2] + stats[:, 3]), axis=0)
    slot_inputs = jnp.sum(arrived[:, :cut].astype(jnp.float32) * share[:, :, None], axis=0)
    slot_inputs = slot_inputs.astype(jnp.bfloat16).reshape(images, own_slots, features)

    rows = lax.all_gather(slot_inputs, "dp", axis=0, tiled=True)
    rows = rows.reshape(ranks * images, experts, per_expert, features)
    rows = rows.transpose(1, 0, 2, 3).reshape(experts, -1, features)
    hidden = jnp.einsum("erd,edf->erf", rows, expert_in, preferred_element_type=jnp.float32)
    hidden = jax.nn.gelu(hidden, approximate=True).astype(jnp.bfloat16)
    result = jnp.einsum("erf,efd->erd", hidden, expert_out, preferred_element_type=jnp.float32)
    result = result.astype(jnp.bfloat16).reshape(experts, ranks, images, per_expert, features)
    result = result.transpose(1, 2, 0, 3, 4).reshape(ranks, images * own_slots, features)
    result = lax.all_to_all(result, "dp", split_axis=0, concat_axis=0, tiled=True)
    outputs = jnp.sum(result.astype(jnp.float32), axis=0).astype(jnp.bfloat16)
    everyone = to_everyone(outputs, OWNERS).reshape(owners, images, own_slots, features)
    everyone = everyone.transpose(1, 0, 2, 3).reshape(images, owners * own_slots, features)

    combined = jnp.einsum("bsm,bsd->bmd", mix, everyone, preferred_element_type=jnp.float32)
    own, right, far, left = (
        combined[:, r * positions : (r + 1) * positions] for r in range(4)
    )
    low = ahead(far[:, :mid].astype(jnp.bfloat16), X, 3)
    high = ahead(far[:, mid:].astype(jnp.bfloat16), X, 1)
    right = right + jnp.pad(low.astype(jnp.float32), ((0, 0), (0, mid), (0, 0)))
    left = left + jnp.pad(high.astype(jnp.float32), ((0, 0), (mid, 0), (0, 0)))
    right = ahead(right.astype(jnp.bfloat16), X, 3)
    left = ahead(left.astype(jnp.bfloat16), X, 1)
    return (own + right.astype(jnp.float32) + left.astype(jnp.float32)).astype(jnp.bfloat16)


def solution(mesh):
    split = Mesh(mesh.devices.reshape(4, 4, 2, mesh.shape["dp"]), (X, Z, Y, "dp"))
    return jax.shard_map(
        shards,
        mesh=split,
        in_specs=(P("dp", SLOT, None), P(None, SLOT), P(SLOT, None, "dp"), P(SLOT, "dp", None)),
        out_specs=P("dp", SLOT, None),
        check_vma=False,
    )
```

```python
import functools

import jax
import jax.numpy as jnp
from jax import lax
from jax.experimental import pallas as pl
from jax.experimental.pallas import tpu as pltpu
from jax.sharding import Mesh
from jax.sharding import PartitionSpec as P


X, Z, Y = "slot_0", "slot_1", "slot_2"
SLOT = (X, Z, Y)
OWNERS = (Z, Y)
LANES = 128
ROOM = 16 * 1024 * 1024
VMEM = pl.BlockSpec(memory_space=pltpu.VMEM)


def ahead(array, axis, step):
    size = lax.axis_size(axis)
    return lax.ppermute(array, axis, [((i + step) % size, i) for i in range(size)])


def all_to_all(array, axis):
    return lax.all_to_all(array, axis, split_axis=0, concat_axis=0, tiled=True)


def to_everyone(array, axis):
    copies = jnp.broadcast_to(array, (lax.axis_size(axis), *array.shape))
    return all_to_all(copies, axis)


def dispatch_kernel(keys, *refs):
    *blocks, message, logits, row_stats = refs
    owners, own_slots, features = keys.shape
    slots = owners * own_slots
    positions = blocks[0].shape[0]
    columns = keys[...].reshape(slots, features)
    for r, block in enumerate(blocks):
        logits[:, r * positions : (r + 1) * positions] = lax.dot_general(
            columns, block[...], (((1,), (1,)), ((), ())), preferred_element_type=jnp.float32
        )
    values = logits[...]
    row_top = jnp.max(values, axis=0, keepdims=True)
    row_stats[0:1] = row_top
    row_stats[1:2] = jnp.sum(jnp.exp(values - row_top), axis=0, keepdims=True)
    top = jnp.max(values, axis=1, keepdims=True).astype(jnp.bfloat16).astype(jnp.float32)
    raised = jnp.exp(values - top)
    rest = jnp.sum(raised, axis=1, keepdims=True)
    lane = lax.broadcasted_iota(jnp.int32, (slots, LANES), 1)
    stats = jnp.where(lane == 0, top, 0.0)
    for k in (1, 2, 3):
        piece = rest.astype(jnp.bfloat16).astype(jnp.float32)
        stats = jnp.where(lane == k, piece, stats)
        rest = rest - piece
    message[:, :, features:] = stats.astype(jnp.bfloat16).reshape(owners, own_slots, LANES)
    weights = raised.astype(jnp.bfloat16)
    sums = None
    for r, block in enumerate(blocks):
        part = jnp.dot(
            weights[:, r * positions : (r + 1) * positions],
            block[...],
            preferred_element_type=jnp.float32,
        )
        sums = part if sums is None else sums + part
    message[:, :, :features] = sums.astype(jnp.bfloat16).reshape(owners, own_slots, features)


def dispatch(keys, blocks):
    owners, own_slots, features = keys.shape
    slots, positions = owners * own_slots, len(blocks) * blocks[0].shape[0]
    return pl.pallas_call(
        dispatch_kernel,
        out_shape=(
            jax.ShapeDtypeStruct((owners, own_slots, features + LANES), jnp.bfloat16),
            jax.ShapeDtypeStruct((slots, positions), jnp.float32),
            jax.ShapeDtypeStruct((2, positions), jnp.float32),
        ),
        in_specs=[VMEM] * (1 + len(blocks)),
        out_specs=(VMEM,) * 3,
        cost_estimate=pl.CostEstimate(
            flops=4 * slots * positions * features,
            bytes_accessed=4 * slots * features,
            transcendentals=2 * slots * positions,
        ),
        compiler_params=pltpu.CompilerParams(vmem_limit_bytes=ROOM),
        name="dispatch",
    )(keys, *blocks)


def merge_kernel(*refs):
    *arrived, inputs = refs
    features = inputs.shape[2]
    for b, pieces in enumerate(arrived):
        owners = pieces.shape[0]
        tops, totals = [], []
        for k in range(owners):
            stats = pieces[k, :, features:].astype(jnp.float32)
            tops.append(stats[:, 0:1])
            totals.append(stats[:, 1:2] + stats[:, 2:3] + stats[:, 3:4])
        peak = functools.reduce(jnp.maximum, tops)
        scales = [jnp.exp(top - peak) for top in tops]
        whole = sum(scale * total for scale, total in zip(scales, totals))
        summed = sum(
            (scales[k] / whole) * pieces[k, :, :features].astype(jnp.float32)
            for k in range(owners)
        )
        inputs[b] = summed.astype(jnp.bfloat16)


def merge(arrived):
    _, own_slots, width = arrived[0].shape
    shape = (len(arrived), own_slots, width - LANES)
    return pl.pallas_call(
        merge_kernel,
        out_shape=jax.ShapeDtypeStruct(shape, jnp.bfloat16),
        in_specs=[VMEM] * len(arrived),
        out_specs=VMEM,
        cost_estimate=pl.CostEstimate(
            flops=1000000, bytes_accessed=2 * len(arrived) * arrived[0].size, transcendentals=0
        ),
        compiler_params=pltpu.CompilerParams(vmem_limit_bytes=ROOM),
        name="merge",
    )(*arrived)


def combine_kernel(logits, own_stats, first, second, third, everyone, own, right, far, left):
    positions = own.shape[0]
    owners, own_slots, features = everyone.shape
    stats = [own_stats[...], first[...], second[...], third[...]]
    for k in (1, 2, 3):
        cut = 4 * positions - k * positions
        stats[k] = jnp.concatenate([stats[k][:, cut:], stats[k][:, :cut]], axis=1)
    highest = functools.reduce(jnp.maximum, [s[0:1] for s in stats])
    whole = sum(s[1:2] * jnp.exp(s[0:1] - highest) for s in stats)
    mix = (jnp.exp(logits[...] - highest) / whole).astype(jnp.bfloat16)
    outputs = everyone[...].reshape(owners * own_slots, features)
    for r, out in enumerate((own, right, far, left)):
        out[...] = lax.dot_general(
            mix[:, r * positions : (r + 1) * positions],
            outputs,
            (((0,), (0,)), ((), ())),
            preferred_element_type=jnp.float32,
        ).astype(out.dtype)


def combine(logits, own_stats, other_stats, everyone):
    slots, width = logits.shape
    features = everyone.shape[2]
    shape = (width // 4, features)
    return pl.pallas_call(
        combine_kernel,
        out_shape=(
            jax.ShapeDtypeStruct(shape, jnp.float32),
            jax.ShapeDtypeStruct(shape, jnp.float32),
            jax.ShapeDtypeStruct(shape, jnp.bfloat16),
            jax.ShapeDtypeStruct(shape, jnp.float32),
        ),
        in_specs=[VMEM] * 6,
        out_specs=(VMEM,) * 4,
        cost_estimate=pl.CostEstimate(
            flops=2 * slots * width * features,
            bytes_accessed=4 * slots * width,
            transcendentals=slots * width,
        ),
        compiler_params=pltpu.CompilerParams(vmem_limit_bytes=ROOM),
        name="combine",
    )(logits, own_stats, *other_stats, everyone)


def shards(tokens, slot_keys, expert_in, expert_out):
    images, positions, features = tokens.shape
    own_slots = slot_keys.shape[1]
    experts = expert_in.shape[0]
    per_expert = own_slots // experts
    ranks = lax.axis_size("dp")
    mid = positions // 2

    keys = to_everyone(slot_keys.T, OWNERS)
    arrived, logits, row_stats = [], [], []
    for b in range(images):
        own = tokens[b]
        right = ahead(own, X, 1)
        left = ahead(own, X, 3)
        if b % 3 == 0:
            far = [ahead(right, X, 1)]
        elif b % 3 == 1:
            far = [ahead(left, X, 3)]
        else:
            far = [ahead(right[:mid], X, 1), ahead(left[mid:], X, 3)]
            far = [jnp.concatenate(far, axis=0)]
        message, values, stats = dispatch(keys, [own, right, *far, left])
        arrived.append(all_to_all(message, OWNERS))
        logits.append(values)
        row_stats.append(stats)
    joint = jnp.stack(row_stats)
    other_stats = [ahead(joint, X, k) for k in (1, 2, 3)]
    slot_inputs = merge(arrived)

    rows = lax.all_gather(slot_inputs, "dp", axis=0, tiled=True)
    rows = rows.reshape(ranks * images, experts, per_expert, features)
    rows = rows.transpose(1, 0, 2, 3).reshape(experts, -1, features)
    hidden = jnp.einsum("erd,edf->erf", rows, expert_in, preferred_element_type=jnp.float32)
    hidden = jax.nn.gelu(hidden, approximate=True).astype(jnp.bfloat16)
    result = jnp.einsum("erf,efd->erd", hidden, expert_out, preferred_element_type=jnp.float32)
    result = result.astype(jnp.bfloat16).reshape(experts, ranks, images, per_expert, features)
    result = result.transpose(1, 2, 0, 3, 4).reshape(ranks, images * own_slots, features)
    result = all_to_all(result, "dp")
    outputs = jnp.sum(result.astype(jnp.float32), axis=0).astype(jnp.bfloat16)
    outputs = outputs.reshape(images, own_slots, features)

    finished = []
    for b in range(images):
        everyone = to_everyone(outputs[b], OWNERS)
        own, right, far, left = combine(
            logits[b], row_stats[b], [o[b] for o in other_stats], everyone
        )
        if b % 3 == 0:
            right = right + ahead(far, X, 3).astype(jnp.float32)
        elif b % 3 == 1:
            left = left + ahead(far, X, 1).astype(jnp.float32)
        else:
            low = ahead(far[:mid], X, 3).astype(jnp.float32)
            high = ahead(far[mid:], X, 1).astype(jnp.float32)
            right = right + jnp.pad(low, ((0, mid), (0, 0)))
            left = left + jnp.pad(high, ((mid, 0), (0, 0)))
        right = ahead(right.astype(jnp.bfloat16), X, 3).astype(jnp.float32)
        left = ahead(left.astype(jnp.bfloat16), X, 1).astype(jnp.float32)
        finished.append((own + right + left).astype(jnp.bfloat16))
    return jnp.stack(finished)


def solution(mesh):
    split = Mesh(mesh.devices.reshape(4, 4, 2, mesh.shape["dp"]), (X, Z, Y, "dp"))
    return jax.shard_map(
        shards,
        mesh=split,
        in_specs=(P("dp", SLOT, None), P(None, SLOT), P(SLOT, None, "dp"), P(SLOT, "dp", None)),
        out_specs=P("dp", SLOT, None),
        check_vma=False,
    )
```

```python
import functools

import jax
import jax.numpy as jnp
from jax import lax
from jax.experimental import pallas as pl
from jax.experimental.pallas import tpu as pltpu
from jax.sharding import Mesh
from jax.sharding import PartitionSpec as P


X, Z, Y = "slot_0", "slot_1", "slot_2"
SLOT = (X, Z, Y)
OWNERS = (Z, Y)
LANES = 128
ROOM = 24 * 1024 * 1024
VMEM = pl.BlockSpec(memory_space=pltpu.VMEM)


def ahead(array, axis, step):
    size = lax.axis_size(axis)
    return lax.ppermute(array, axis, [((i + step) % size, i) for i in range(size)])


def swapped(array, axis, mask):
    size = lax.axis_size(axis)
    return lax.ppermute(array, axis, [(i, i ^ mask) for i in range(size)])


def all_to_all(array, axis):
    return lax.all_to_all(array, axis, split_axis=0, concat_axis=0, tiled=True)


def to_everyone(array, axis):
    copies = jnp.broadcast_to(array, (lax.axis_size(axis), *array.shape))
    return all_to_all(copies, axis)


def dispatch_kernel(keys, own, r0, r1, f0, f1, l0, l1, message, logits, row_stats, field):
    owners, own_slots, features = keys.shape
    slots = owners * own_slots
    images, positions, _ = own.shape
    half = positions // 2

    def one(b, carry):
        field[:positions] = own[b]
        for k, block in enumerate((r0, r1, f0, f1, l0, l1)):
            field[positions + k * half : positions + (k + 1) * half] = block[b]
        values = lax.dot_general(
            keys[...].reshape(slots, features),
            field[...],
            (((1,), (1,)), ((), ())),
            preferred_element_type=jnp.float32,
        )
        logits[b] = values
        row_top = jnp.max(values, axis=0, keepdims=True)
        row_total = jnp.sum(jnp.exp(values - row_top), axis=0, keepdims=True)
        row_stats[b] = jnp.concatenate([row_top, row_total], axis=0)
        top = jnp.max(values, axis=1, keepdims=True).astype(jnp.bfloat16).astype(jnp.float32)
        raised = jnp.exp(values - top)
        rest = jnp.sum(raised, axis=1, keepdims=True)
        lane = lax.broadcasted_iota(jnp.int32, (slots, LANES), 1)
        stats = jnp.where(lane == 0, top, 0.0)
        for k in (1, 2, 3):
            piece = rest.astype(jnp.bfloat16).astype(jnp.float32)
            stats = jnp.where(lane == k, piece, stats)
            rest = rest - piece
        stats = stats.astype(jnp.bfloat16).reshape(owners, own_slots, LANES)
        sums = jnp.dot(
            raised.astype(jnp.bfloat16), field[...], preferred_element_type=jnp.float32
        ).astype(jnp.bfloat16)
        sums = sums.reshape(owners, own_slots, features)
        for k in range(owners):
            message[k, b, :, features:] = stats[k]
            message[k, b, :, :features] = sums[k]
        return carry

    lax.fori_loop(0, images, one, 0)


def dispatch(keys, blocks):
    owners, own_slots, features = keys.shape
    images = blocks[0].shape[0]
    slots, positions = owners * own_slots, sum(block.shape[1] for block in blocks)
    return pl.pallas_call(
        dispatch_kernel,
        out_shape=(
            jax.ShapeDtypeStruct((owners, images, own_slots, features + LANES), jnp.bfloat16),
            jax.ShapeDtypeStruct((images, slots, positions), jnp.float32),
            jax.ShapeDtypeStruct((images, 2, positions), jnp.float32),
        ),
        in_specs=[VMEM] * (1 + len(blocks)),
        out_specs=(VMEM,) * 3,
        scratch_shapes=[pltpu.VMEM((positions, features), jnp.bfloat16)],
        cost_estimate=pl.CostEstimate(
            flops=4 * images * slots * positions * features,
            bytes_accessed=4 * images * slots * features,
            transcendentals=2 * images * slots * positions,
        ),
        compiler_params=pltpu.CompilerParams(vmem_limit_bytes=ROOM),
        name="dispatch",
    )(keys, *blocks)


def merge_kernel(arrived, inputs):
    owners, images, _, _ = arrived.shape
    features = inputs.shape[2]
    for b in range(images):
        tops, totals = [], []
        for k in range(owners):
            stats = arrived[k, b, :, features:].astype(jnp.float32)
            tops.append(stats[:, 0:1])
            totals.append(stats[:, 1:2] + stats[:, 2:3] + stats[:, 3:4])
        peak = functools.reduce(jnp.maximum, tops)
        scales = [jnp.exp(top - peak) for top in tops]
        whole = sum(scale * total for scale, total in zip(scales, totals))
        summed = sum(
            (scales[k] / whole) * arrived[k, b, :, :features].astype(jnp.float32)
            for k in range(owners)
        )
        inputs[b] = summed.astype(jnp.bfloat16)


def merge(arrived):
    _, images, own_slots, width = arrived.shape
    return pl.pallas_call(
        merge_kernel,
        out_shape=jax.ShapeDtypeStruct((images, own_slots, width - LANES), jnp.bfloat16),
        in_specs=[VMEM],
        out_specs=VMEM,
        cost_estimate=pl.CostEstimate(
            flops=4 * arrived.size, bytes_accessed=2 * arrived.size, transcendentals=0
        ),
        compiler_params=pltpu.CompilerParams(vmem_limit_bytes=ROOM),
        name="merge",
    )(arrived)


def combine_kernel(logits, own_stats, first, second, third, everyone, own, *rest):
    images, positions, _ = own.shape
    half = positions // 2
    owners, _, _, _ = everyone.shape

    def one(b, carry):
        stats = [own_stats[b], first[b], second[b], third[b]]
        for k in (1, 2, 3):
            cut = 4 * positions - k * positions
            stats[k] = jnp.concatenate([stats[k][:, cut:], stats[k][:, :cut]], axis=1)
        highest = functools.reduce(jnp.maximum, [s[0:1] for s in stats])
        whole = sum(s[1:2] * jnp.exp(s[0:1] - highest) for s in stats)
        mix = (jnp.exp(logits[b] - highest) / whole).astype(jnp.bfloat16)
        outputs = jnp.concatenate([everyone[k, b] for k in range(owners)], axis=0)
        combined = lax.dot_general(
            mix, outputs, (((0,), (0,)), ((), ())), preferred_element_type=jnp.float32
        )
        own[b] = combined[:positions]
        for k, out in enumerate(rest):
            at = positions + k * half
            out[b] = combined[at : at + half].astype(out.dtype)
        return carry

    lax.fori_loop(0, images, one, 0)


def combine(logits, own_stats, other_stats, everyone):
    images, slots, width = logits.shape
    features = everyone.shape[3]
    positions = width // 4
    kinds = (jnp.float32, jnp.bfloat16, jnp.bfloat16, jnp.bfloat16, jnp.bfloat16, jnp.float32)
    return pl.pallas_call(
        combine_kernel,
        out_shape=(
            jax.ShapeDtypeStruct((images, positions, features), jnp.float32),
            *(jax.ShapeDtypeStruct((images, positions // 2, features), kind) for kind in kinds),
        ),
        in_specs=[VMEM] * 6,
        out_specs=(VMEM,) * 7,
        cost_estimate=pl.CostEstimate(
            flops=2 * images * slots * width * features,
            bytes_accessed=4 * images * slots * width,
            transcendentals=images * slots * width,
        ),
        compiler_params=pltpu.CompilerParams(vmem_limit_bytes=ROOM),
        name="combine",
    )(logits, own_stats, *other_stats, everyone)


def shards(tokens, slot_keys, expert_in, expert_out):
    images, positions, features = tokens.shape
    own_slots = slot_keys.shape[1]
    experts = expert_in.shape[0]
    per_expert = own_slots // experts
    ranks = lax.axis_size("dp")
    half = positions // 2
    low, high = tokens[:, :half], tokens[:, half:]

    r0 = ahead(low, X, 1)
    l1 = ahead(high, X, 3)
    r1 = ahead(high, X, 1)
    l0 = ahead(low, X, 3)
    keys = to_everyone(slot_keys.T, OWNERS)
    f0 = ahead(r0, X, 1)
    f1 = ahead(l1, X, 3)
    message, logits, row_stats = dispatch(keys, [tokens, r0, r1, f0, f1, l0, l1])
    arrived = all_to_all(message, OWNERS)
    other_stats = [ahead(row_stats, X, k) for k in (1, 2, 3)]
    slot_inputs = merge(arrived)

    rows = lax.all_gather(slot_inputs, "dp", axis=0, tiled=True)
    rows = rows.reshape(ranks * images, experts, per_expert, features)
    rows = rows.transpose(1, 0, 2, 3).reshape(experts, -1, features)
    hidden = jnp.einsum("erd,edf->erf", rows, expert_in, preferred_element_type=jnp.float32)
    hidden = jax.nn.gelu(hidden, approximate=True).astype(jnp.bfloat16)
    result = jnp.einsum("erf,efd->erd", hidden, expert_out, preferred_element_type=jnp.float32)
    result = result.reshape(experts, ranks, images, per_expert, features)
    result = result.transpose(1, 2, 0, 3, 4).reshape(ranks, images, own_slots, features)
    rank = lax.axis_index("dp")
    outputs = lax.dynamic_index_in_dim(result, rank, 0, keepdims=False)
    for k in (2, 3, 1):
        piece = lax.dynamic_index_in_dim(result, rank ^ k, 0, keepdims=False)
        piece = swapped(piece.astype(jnp.bfloat16), "dp", k)
        outputs = outputs + piece.astype(jnp.float32)
    everyone = to_everyone(outputs.astype(jnp.bfloat16), OWNERS)

    own, r0, r1, f0, f1, l0, l1 = combine(logits, row_stats, other_stats, everyone)
    p0 = ahead(f0, X, 3).astype(jnp.float32)
    p1 = ahead(f1, X, 1).astype(jnp.float32)
    u1 = ahead(r1, X, 3).astype(jnp.float32)
    v0 = ahead(l0, X, 1).astype(jnp.float32)
    u0 = ahead((r0 + p0).astype(jnp.bfloat16), X, 3).astype(jnp.float32)
    v1 = ahead((l1 + p1).astype(jnp.bfloat16), X, 1).astype(jnp.float32)
    low = (own[:, :half] + u0 + v0).astype(jnp.bfloat16)
    high = (own[:, half:] + u1 + v1).astype(jnp.bfloat16)
    return jnp.concatenate([low, high], axis=1)


def solution(mesh):
    split = Mesh(mesh.devices.reshape(4, 4, 2, mesh.shape["dp"]), (X, Z, Y, "dp"))
    return jax.shard_map(
        shards,
        mesh=split,
        in_specs=(P("dp", SLOT, None), P(None, SLOT), P(SLOT, None, "dp"), P(SLOT, "dp", None)),
        out_specs=P("dp", SLOT, None),
        check_vma=False,
    )
```

```python
import functools

import jax
import jax.numpy as jnp
from jax import lax
from jax.experimental import pallas as pl
from jax.experimental.pallas import tpu as pltpu
from jax.sharding import Mesh
from jax.sharding import PartitionSpec as P


X, Z, Y = "slot_0", "slot_1", "slot_2"
SLOT = (X, Z, Y)
OWNERS = (Z, Y)
LANES = 128
ROOM = 24 * 1024 * 1024
VMEM = pl.BlockSpec(memory_space=pltpu.VMEM)
ANY = pl.BlockSpec(memory_space=pl.ANY)


def ahead(array, axis, step):
    size = lax.axis_size(axis)
    return lax.ppermute(array, axis, [((i + step) % size, i) for i in range(size)])


def swapped(array, axis, mask):
    size = lax.axis_size(axis)
    return lax.ppermute(array, axis, [(i, i ^ mask) for i in range(size)])


def all_to_all(array, axis):
    return lax.all_to_all(array, axis, split_axis=0, concat_axis=0, tiled=True)


def to_everyone(array, axis):
    copies = jnp.broadcast_to(array, (lax.axis_size(axis), *array.shape))
    return all_to_all(copies, axis)


def dispatch_kernel(
    first,
    second,
    keys,
    own,
    r0,
    r1,
    f0,
    f1,
    l0,
    l1,
    message,
    logits,
    row_stats,
    first_here,
    second_here,
    field,
    arrivals,
    loaded,
):
    owners, own_slots, features = keys.shape
    slots = owners * own_slots
    images, positions, _ = own.shape
    half = positions // 2

    def copies(b):
        blocks = [(own.at[b], field.at[b, 0:positions])]
        for k, block in enumerate((r0, r1, f0, f1, l0, l1)):
            at = positions + k * half
            blocks.append((block.at[b], field.at[b, at : at + half]))
        return [
            pltpu.make_async_copy(source, target, arrivals.at[b, k])
            for k, (source, target) in enumerate(blocks)
        ]

    for b in range(images):
        for copy in copies(b):
            copy.start()
    loads = [
        pltpu.make_async_copy(first, first_here, loaded.at[0]),
        pltpu.make_async_copy(second, second_here, loaded.at[1]),
    ]
    for load in loads:
        load.start()

    def one(b, carry):
        for copy in copies(b):
            copy.wait()
        values = lax.dot_general(
            keys[...].reshape(slots, features),
            field[b],
            (((1,), (1,)), ((), ())),
            preferred_element_type=jnp.float32,
        )
        logits[b] = values
        row_top = jnp.max(values, axis=0, keepdims=True)
        row_total = jnp.sum(jnp.exp(values - row_top), axis=0, keepdims=True)
        row_stats[b] = jnp.concatenate([row_top, row_total], axis=0)
        top = jnp.max(values, axis=1, keepdims=True).astype(jnp.bfloat16).astype(jnp.float32)
        raised = jnp.exp(values - top)
        rest = jnp.sum(raised, axis=1, keepdims=True)
        lane = lax.broadcasted_iota(jnp.int32, (slots, LANES), 1)
        stats = jnp.where(lane == 0, top, 0.0)
        for k in (1, 2, 3):
            piece = rest.astype(jnp.bfloat16).astype(jnp.float32)
            stats = jnp.where(lane == k, piece, stats)
            rest = rest - piece
        stats = stats.astype(jnp.bfloat16).reshape(owners, own_slots, LANES)
        sums = jnp.dot(
            raised.astype(jnp.bfloat16), field[b], preferred_element_type=jnp.float32
        ).astype(jnp.bfloat16)
        sums = sums.reshape(owners, own_slots, features)
        for k in range(owners):
            message[k, b, :, features:] = stats[k]
            message[k, b, :, :features] = sums[k]
        return carry

    lax.fori_loop(0, images, one, 0)
    for load in loads:
        load.wait()


def dispatch(weights, keys, blocks):
    owners, own_slots, features = keys.shape
    images = blocks[0].shape[0]
    slots, positions = owners * own_slots, sum(block.shape[1] for block in blocks)
    return pl.pallas_call(
        dispatch_kernel,
        out_shape=(
            jax.ShapeDtypeStruct((owners, images, own_slots, features + LANES), jnp.bfloat16),
            jax.ShapeDtypeStruct((images, slots, positions), jnp.float32),
            jax.ShapeDtypeStruct((images, 2, positions), jnp.float32),
            *(jax.ShapeDtypeStruct(w.shape, w.dtype) for w in weights),
        ),
        in_specs=[ANY] * 2 + [VMEM] + [ANY] * len(blocks),
        out_specs=(VMEM,) * 5,
        scratch_shapes=[
            pltpu.VMEM((images, positions, features), jnp.bfloat16),
            pltpu.SemaphoreType.DMA((images, len(blocks))),
            pltpu.SemaphoreType.DMA((2,)),
        ],
        cost_estimate=pl.CostEstimate(
            flops=4 * images * slots * positions * features,
            bytes_accessed=4 * images * slots * features,
            transcendentals=2 * images * slots * positions,
        ),
        compiler_params=pltpu.CompilerParams(vmem_limit_bytes=ROOM),
        name="dispatch",
    )(*weights, keys, *blocks)


def merge_kernel(arrived, inputs):
    owners, images, _, _ = arrived.shape
    features = inputs.shape[2]
    for b in range(images):
        tops, totals = [], []
        for k in range(owners):
            stats = arrived[k, b, :, features:].astype(jnp.float32)
            tops.append(stats[:, 0:1])
            totals.append(stats[:, 1:2] + stats[:, 2:3] + stats[:, 3:4])
        peak = functools.reduce(jnp.maximum, tops)
        scales = [jnp.exp(top - peak) for top in tops]
        whole = sum(scale * total for scale, total in zip(scales, totals))
        summed = sum(
            (scales[k] / whole) * arrived[k, b, :, :features].astype(jnp.float32)
            for k in range(owners)
        )
        inputs[b] = summed.astype(jnp.bfloat16)


def merge(arrived):
    _, images, own_slots, width = arrived.shape
    return pl.pallas_call(
        merge_kernel,
        out_shape=jax.ShapeDtypeStruct((images, own_slots, width - LANES), jnp.bfloat16),
        in_specs=[VMEM],
        out_specs=VMEM,
        cost_estimate=pl.CostEstimate(
            flops=4 * arrived.size, bytes_accessed=2 * arrived.size, transcendentals=0
        ),
        compiler_params=pltpu.CompilerParams(vmem_limit_bytes=ROOM),
        name="merge",
    )(arrived)


def expert_kernel(rows, first, second, *outs):
    rank = lax.axis_index("dp")
    experts = first.shape[0]
    images, own_slots, _ = outs[0].shape
    per_expert = own_slots // experts

    def one(expert, carry):
        cut = pl.ds(pl.multiple_of(expert * per_expert, per_expert), per_expert)
        taken = [
            rows[(rank ^ k) * images + b, cut, :]
            for k in range(len(outs))
            for b in range(images)
        ]
        hidden = jnp.dot(
            jnp.concatenate(taken, axis=0), first[expert], preferred_element_type=jnp.float32
        )
        hidden = jax.nn.gelu(hidden, approximate=True).astype(jnp.bfloat16)
        result = jnp.dot(hidden, second[expert], preferred_element_type=jnp.float32)
        for k, out in enumerate(outs):
            for b in range(images):
                at = (k * images + b) * per_expert
                out[b, cut, :] = result[at : at + per_expert].astype(out.dtype)
        return carry

    lax.fori_loop(0, experts, one, 0)


def run_experts(rows, expert_in, expert_out, ranks):
    images, own_slots = rows.shape[0] // ranks, rows.shape[1]
    shape = (images, own_slots, rows.shape[2])
    kinds = (jnp.float32, *(jnp.bfloat16 for _ in range(ranks - 1)))
    return pl.pallas_call(
        expert_kernel,
        out_shape=[jax.ShapeDtypeStruct(shape, kind) for kind in kinds],
        in_specs=[VMEM] * 3,
        out_specs=[VMEM] * ranks,
        cost_estimate=pl.CostEstimate(
            flops=4 * rows.size * expert_in.shape[2],
            bytes_accessed=4 * expert_in.size,
            transcendentals=rows.size,
        ),
        compiler_params=pltpu.CompilerParams(vmem_limit_bytes=ROOM),
        name="experts",
    )(rows, expert_in, expert_out)


def spread_kernel(own, first, second, third, copies):
    total = own[...]
    for piece in (first, second, third):
        total = total + piece[...].astype(jnp.float32)
    total = total.astype(jnp.bfloat16)
    for k in range(copies.shape[0]):
        copies[k] = total


def spread(own, pieces, count):
    return pl.pallas_call(
        spread_kernel,
        out_shape=jax.ShapeDtypeStruct((count, *own.shape), jnp.bfloat16),
        in_specs=[VMEM] * 4,
        out_specs=VMEM,
        cost_estimate=pl.CostEstimate(
            flops=4 * own.size, bytes_accessed=2 * count * own.size, transcendentals=0
        ),
        compiler_params=pltpu.CompilerParams(vmem_limit_bytes=ROOM),
        name="spread",
    )(own, *pieces)


def combine_kernel(logits, own_stats, first, second, third, everyone, own, *rest):
    images, positions, _ = own.shape
    half = positions // 2
    owners, _, _, _ = everyone.shape

    def one(b, carry):
        stats = [own_stats[b], first[b], second[b], third[b]]
        for k in (1, 2, 3):
            cut = 4 * positions - k * positions
            stats[k] = jnp.concatenate([stats[k][:, cut:], stats[k][:, :cut]], axis=1)
        highest = functools.reduce(jnp.maximum, [s[0:1] for s in stats])
        whole = sum(s[1:2] * jnp.exp(s[0:1] - highest) for s in stats)
        mix = (jnp.exp(logits[b] - highest) / whole).astype(jnp.bfloat16)
        outputs = jnp.concatenate([everyone[k, b] for k in range(owners)], axis=0)
        combined = lax.dot_general(
            mix, outputs, (((0,), (0,)), ((), ())), preferred_element_type=jnp.float32
        )
        own[b] = combined[:positions]
        for k, out in enumerate(rest):
            at = positions + k * half
            out[b] = combined[at : at + half].astype(out.dtype)
        return carry

    lax.fori_loop(0, images, one, 0)


def combine(logits, own_stats, other_stats, everyone):
    images, slots, width = logits.shape
    features = everyone.shape[3]
    positions = width // 4
    kinds = (jnp.float32, jnp.bfloat16, jnp.bfloat16, jnp.bfloat16, jnp.bfloat16, jnp.float32)
    return pl.pallas_call(
        combine_kernel,
        out_shape=(
            jax.ShapeDtypeStruct((images, positions, features), jnp.float32),
            *(jax.ShapeDtypeStruct((images, positions // 2, features), kind) for kind in kinds),
        ),
        in_specs=[VMEM] * 6,
        out_specs=(VMEM,) * 7,
        cost_estimate=pl.CostEstimate(
            flops=2 * images * slots * width * features,
            bytes_accessed=4 * images * slots * width,
            transcendentals=images * slots * width,
        ),
        compiler_params=pltpu.CompilerParams(vmem_limit_bytes=ROOM),
        name="combine",
    )(logits, own_stats, *other_stats, everyone)


def shards(tokens, slot_keys, expert_in, expert_out):
    _, positions, _ = tokens.shape
    ranks = lax.axis_size("dp")
    half = positions // 2
    low, high = tokens[:, :half], tokens[:, half:]

    r0 = ahead(low, X, 1)
    l1 = ahead(high, X, 3)
    r1 = ahead(high, X, 1)
    l0 = ahead(low, X, 3)
    keys = to_everyone(slot_keys.T, OWNERS)
    f0 = ahead(r0, X, 1)
    f1 = ahead(l1, X, 3)
    message, logits, row_stats, *weights = dispatch(
        (expert_in, expert_out), keys, [tokens, r0, r1, f0, f1, l0, l1]
    )
    arrived = all_to_all(message, OWNERS)
    rows = lax.all_gather(merge(arrived), "dp", axis=0, tiled=True)
    row_stats, rows = lax.optimization_barrier((row_stats, rows))
    other_stats = [ahead(row_stats, X, k) for k in (1, 2, 3)]
    own, *pieces = run_experts(rows, *weights, ranks)
    pieces = [swapped(piece, "dp", k) for k, piece in zip((1, 2, 3), pieces)]
    pieces, other_stats = lax.optimization_barrier((pieces, other_stats))
    everyone = all_to_all(spread(own, pieces, lax.axis_size(OWNERS)), OWNERS)

    own, r0, r1, f0, f1, l0, l1 = combine(logits, row_stats, other_stats, everyone)
    p0 = ahead(f0, X, 3).astype(jnp.float32)
    p1 = ahead(f1, X, 1).astype(jnp.float32)
    u1 = ahead(r1, X, 3).astype(jnp.float32)
    v0 = ahead(l0, X, 1).astype(jnp.float32)
    u0 = ahead((r0 + p0).astype(jnp.bfloat16), X, 3).astype(jnp.float32)
    v1 = ahead((l1 + p1).astype(jnp.bfloat16), X, 1).astype(jnp.float32)
    low = (own[:, :half] + u0 + v0).astype(jnp.bfloat16)
    high = (own[:, half:] + u1 + v1).astype(jnp.bfloat16)
    return jnp.concatenate([low, high], axis=1)


def solution(mesh):
    split = Mesh(mesh.devices.reshape(4, 4, 2, mesh.shape["dp"]), (X, Z, Y, "dp"))
    return jax.shard_map(
        shards,
        mesh=split,
        in_specs=(P("dp", SLOT, None), P(None, SLOT), P(SLOT, None, "dp"), P(SLOT, "dp", None)),
        out_specs=P("dp", SLOT, None),
        check_vma=False,
    )
```

```python
import functools

import jax
import jax.numpy as jnp
from jax import lax
from jax.experimental import pallas as pl
from jax.experimental.pallas import tpu as pltpu
from jax.sharding import Mesh
from jax.sharding import PartitionSpec as P


X, Z, Y = "slot_0", "slot_1", "slot_2"
SLOT = (X, Z, Y)
TILE = tuple(
    tuple((x * 4 + z) * 2 + y for x in range(4) for z in range(4) if (x + 2 * z) % 4 == r for y in (0, 1))
    for r in range(4)
)
LANES = 128
ROOM = 24 * 1024 * 1024
VMEM = pl.BlockSpec(memory_space=pltpu.VMEM)
ANY = pl.BlockSpec(memory_space=pl.ANY)


def ahead(array, axis, step):
    size = lax.axis_size(axis)
    return lax.ppermute(array, axis, [((i + step) % size, i) for i in range(size)])


def swapped(array, axis, mask):
    size = lax.axis_size(axis)
    return lax.ppermute(array, axis, [(i, i ^ mask) for i in range(size)])


def all_to_all(array):
    return lax.all_to_all(
        array, SLOT, split_axis=0, concat_axis=0, axis_index_groups=TILE, tiled=True
    )


def dispatch_kernel(keys, first, *refs):
    *blocks, message, logits, s0, s1, s2, s3, first_here, field, arrivals, loaded = refs
    owners, own_slots, features = keys.shape
    slots = owners * own_slots
    images, positions, _ = blocks[0].shape

    def copies(b):
        return [
            pltpu.make_async_copy(
                block.at[b], field.at[b, k * positions : (k + 1) * positions], arrivals.at[b, k]
            )
            for k, block in enumerate(blocks)
        ]

    for b in range(images):
        for copy in copies(b):
            copy.start()
    load = pltpu.make_async_copy(first, first_here, loaded)
    load.start()

    def one(b, carry):
        for copy in copies(b):
            copy.wait()
        values = lax.dot_general(
            keys[...].reshape(slots, features),
            field[b],
            (((1,), (1,)), ((), ())),
            preferred_element_type=jnp.float32,
        )
        logits[b] = values
        row_top = jnp.max(values, axis=0, keepdims=True)
        row_total = jnp.sum(jnp.exp(values - row_top), axis=0, keepdims=True)
        row_stats = jnp.concatenate([row_top, row_total], axis=0)
        for k, out in enumerate((s0, s1, s2, s3)):
            out[b] = row_stats[:, k * positions : (k + 1) * positions]
        top = jnp.max(values, axis=1, keepdims=True).astype(jnp.bfloat16).astype(jnp.float32)
        raised = jnp.exp(values - top)
        rest = jnp.sum(raised, axis=1, keepdims=True)
        lane = lax.broadcasted_iota(jnp.int32, (slots, LANES), 1)
        stats = jnp.where(lane == 0, top, 0.0)
        for k in (1, 2, 3):
            piece = rest.astype(jnp.bfloat16).astype(jnp.float32)
            stats = jnp.where(lane == k, piece, stats)
            rest = rest - piece
        stats = stats.astype(jnp.bfloat16).reshape(owners, own_slots, LANES)
        sums = jnp.dot(
            raised.astype(jnp.bfloat16), field[b], preferred_element_type=jnp.float32
        ).astype(jnp.bfloat16)
        sums = sums.reshape(owners, own_slots, features)
        for k in range(owners):
            message[k, b, :, features:] = stats[k]
            message[k, b, :, :features] = sums[k]
        return carry

    lax.fori_loop(0, images, one, 0)
    load.wait()


def dispatch(keys, first, blocks):
    owners, own_slots, features = keys.shape
    images, positions, _ = blocks[0].shape
    slots, width = owners * own_slots, len(blocks) * positions
    return pl.pallas_call(
        dispatch_kernel,
        out_shape=(
            jax.ShapeDtypeStruct((owners, images, own_slots, features + LANES), jnp.bfloat16),
            jax.ShapeDtypeStruct((images, slots, width), jnp.float32),
            *(jax.ShapeDtypeStruct((images, 2, positions), jnp.float32) for _ in blocks),
            jax.ShapeDtypeStruct(first.shape, first.dtype),
        ),
        in_specs=[VMEM] + [ANY] * (1 + len(blocks)),
        out_specs=(VMEM,) * (3 + len(blocks)),
        scratch_shapes=[
            pltpu.VMEM((images, width, features), jnp.bfloat16),
            pltpu.SemaphoreType.DMA((images, len(blocks))),
            pltpu.SemaphoreType.DMA,
        ],
        cost_estimate=pl.CostEstimate(
            flops=4 * images * slots * width * features,
            bytes_accessed=4 * images * slots * features,
            transcendentals=2 * images * slots * width,
        ),
        compiler_params=pltpu.CompilerParams(vmem_limit_bytes=32 * 1024 * 1024),
        name="dispatch",
    )(keys, first, *blocks)


def merge_kernel(arrived, inputs):
    owners, images, _, _ = arrived.shape
    features = inputs.shape[2]
    for b in range(images):
        tops, totals = [], []
        for k in range(owners):
            stats = arrived[k, b, :, features:].astype(jnp.float32)
            tops.append(stats[:, 0:1])
            totals.append(stats[:, 1:2] + stats[:, 2:3] + stats[:, 3:4])
        peak = functools.reduce(jnp.maximum, tops)
        scales = [jnp.exp(top - peak) for top in tops]
        whole = sum(scale * total for scale, total in zip(scales, totals))
        summed = sum(
            (scales[k] / whole) * arrived[k, b, :, :features].astype(jnp.float32)
            for k in range(owners)
        )
        inputs[b] = summed.astype(jnp.bfloat16)


def merge(arrived):
    _, images, own_slots, width = arrived.shape
    return pl.pallas_call(
        merge_kernel,
        out_shape=jax.ShapeDtypeStruct((images, own_slots, width - LANES), jnp.bfloat16),
        in_specs=[VMEM],
        out_specs=VMEM,
        cost_estimate=pl.CostEstimate(
            flops=4 * arrived.size, bytes_accessed=2 * arrived.size, transcendentals=0
        ),
        compiler_params=pltpu.CompilerParams(vmem_limit_bytes=ROOM),
        name="merge",
    )(arrived)


def expert_kernel(rows, first, second, *refs):
    *outs, second_here, loaded = refs
    rank = lax.axis_index("dp")
    experts = first.shape[0]
    images, own_slots, _ = outs[0].shape
    per_expert = own_slots // experts

    def load(expert):
        return pltpu.make_async_copy(second.at[expert], second_here.at[expert], loaded.at[expert])

    for expert in range(experts):
        load(expert).start()

    def one(expert, carry):
        cut = pl.ds(pl.multiple_of(expert * per_expert, per_expert), per_expert)
        taken = [
            rows[(rank ^ k) * images + b, cut, :]
            for k in range(len(outs))
            for b in range(images)
        ]
        hidden = jnp.dot(
            jnp.concatenate(taken, axis=0), first[expert], preferred_element_type=jnp.float32
        )
        hidden = jax.nn.gelu(hidden, approximate=True).astype(jnp.bfloat16)
        load(expert).wait()
        result = jnp.dot(hidden, second_here[expert], preferred_element_type=jnp.float32)
        for k, out in enumerate(outs):
            for b in range(images):
                at = (k * images + b) * per_expert
                out[b, cut, :] = result[at : at + per_expert].astype(out.dtype)
        return carry

    lax.fori_loop(0, experts, one, 0)


def run_experts(rows, expert_in, expert_out, ranks):
    images, own_slots = rows.shape[0] // ranks, rows.shape[1]
    shape = (images, own_slots, rows.shape[2])
    kinds = (jnp.float32, *(jnp.bfloat16 for _ in range(ranks - 1)))
    return pl.pallas_call(
        expert_kernel,
        out_shape=[jax.ShapeDtypeStruct(shape, kind) for kind in kinds],
        in_specs=[VMEM, VMEM, ANY],
        out_specs=[VMEM] * ranks,
        scratch_shapes=[
            pltpu.VMEM(expert_out.shape, expert_out.dtype),
            pltpu.SemaphoreType.DMA((expert_out.shape[0],)),
        ],
        cost_estimate=pl.CostEstimate(
            flops=4 * rows.size * expert_in.shape[2],
            bytes_accessed=4 * expert_in.size,
            transcendentals=rows.size,
        ),
        compiler_params=pltpu.CompilerParams(vmem_limit_bytes=ROOM),
        name="experts",
    )(rows, expert_in, expert_out)


def spread_kernel(own, first, second, third, copies):
    total = own[...]
    for piece in (first, second, third):
        total = total + piece[...].astype(jnp.float32)
    total = total.astype(jnp.bfloat16)
    for k in range(copies.shape[0]):
        copies[k] = total


def spread(own, pieces, count):
    return pl.pallas_call(
        spread_kernel,
        out_shape=jax.ShapeDtypeStruct((count, *own.shape), jnp.bfloat16),
        in_specs=[VMEM] * 4,
        out_specs=VMEM,
        cost_estimate=pl.CostEstimate(
            flops=4 * own.size, bytes_accessed=2 * count * own.size, transcendentals=0
        ),
        compiler_params=pltpu.CompilerParams(vmem_limit_bytes=ROOM),
        name="spread",
    )(own, *pieces)


def combine_kernel(logits, everyone, *refs):
    stats, outs = refs[:4], refs[4:]
    images, positions, _ = outs[0].shape
    owners = everyone.shape[0]

    def one(b, carry):
        outputs = jnp.concatenate([everyone[k, b] for k in range(owners)], axis=0)
        for r in (3, 1, 2, 0):
            values = logits[b, :, r * positions : (r + 1) * positions]
            mix = jnp.exp(values - stats[r][b][0:1]).astype(jnp.bfloat16)
            outs[r][b] = lax.dot_general(
                mix, outputs, (((0,), (0,)), ((), ())), preferred_element_type=jnp.float32
            ).astype(outs[r].dtype)
        return carry

    lax.fori_loop(0, images, one, 0)


def combine(logits, everyone, stats):
    images, slots, width = logits.shape
    shape = (images, width // len(stats), everyone.shape[3])
    kinds = (jnp.float32, jnp.bfloat16, jnp.bfloat16, jnp.bfloat16)
    return pl.pallas_call(
        combine_kernel,
        out_shape=[jax.ShapeDtypeStruct(shape, kind) for kind in kinds],
        in_specs=[VMEM] * (2 + len(stats)),
        out_specs=(VMEM,) * len(kinds),
        cost_estimate=pl.CostEstimate(
            flops=2 * images * slots * width * shape[2],
            bytes_accessed=4 * images * slots * width,
            transcendentals=images * slots * width,
        ),
        compiler_params=pltpu.CompilerParams(vmem_limit_bytes=ROOM),
        name="combine",
    )(logits, everyone, *stats)


def finish_kernel(*refs):
    parts, stats, out = refs[:4], refs[4:8], refs[8]
    images, positions, _ = out.shape
    for b in range(images):
        tops = [s[b][0:1] for s in stats]
        highest = functools.reduce(jnp.maximum, tops)
        scales = [jnp.exp(top - highest) for top in tops]
        total = sum(scale * s[b][1:2] for scale, s in zip(scales, stats))
        shares = [scale / total for scale in scales]
        shares = jnp.concatenate(shares + [jnp.zeros((LANES - 4, positions), jnp.float32)], axis=0)
        shares = shares.T
        joined = sum(
            shares[:, k : k + 1] * part[b].astype(jnp.float32) for k, part in enumerate(parts)
        )
        out[b] = joined.astype(out.dtype)


def finish(parts, stats):
    shape = parts[0].shape
    return pl.pallas_call(
        finish_kernel,
        out_shape=jax.ShapeDtypeStruct(shape, jnp.bfloat16),
        in_specs=[VMEM] * 8,
        out_specs=VMEM,
        cost_estimate=pl.CostEstimate(
            flops=8 * parts[0].size, bytes_accessed=12 * parts[0].size, transcendentals=0
        ),
        compiler_params=pltpu.CompilerParams(vmem_limit_bytes=ROOM),
        name="finish",
    )(*parts, *stats)


def shards(tokens, slot_keys, expert_in, expert_out):
    ranks = lax.axis_size("dp")
    owners = len(TILE[0])
    near = [ahead(tokens, X, 1), ahead(tokens, X, 3), ahead(tokens, Z, 1)]
    keys = all_to_all(jnp.broadcast_to(slot_keys.T, (owners, *slot_keys.shape[::-1])))
    message, logits, *stats, first = dispatch(keys, expert_in, [tokens, *near])
    arrived = all_to_all(message)
    rows = lax.all_gather(merge(arrived), "dp", axis=0, tiled=True)
    away, rows = lax.optimization_barrier((stats[1:], rows))
    back = [ahead(away[0], X, 3), ahead(away[1], X, 1), ahead(away[2], Z, 3)]
    own, *pieces = run_experts(rows, first, expert_out, ranks)
    pieces = [swapped(piece, "dp", k) for k, piece in zip((1, 2, 3), pieces)]
    pieces, back = lax.optimization_barrier((pieces, back))
    everyone = all_to_all(spread(own, pieces, owners))
    own, right, left, up = combine(logits, everyone, stats)
    parts = [own, ahead(right, X, 3), ahead(left, X, 1), ahead(up, Z, 3)]
    return finish(parts, [stats[0], *back])


def solution(mesh):
    split = Mesh(mesh.devices.reshape(4, 4, 2, mesh.shape["dp"]), (X, Z, Y, "dp"))
    return jax.shard_map(
        shards,
        mesh=split,
        in_specs=(P("dp", SLOT, None), P(None, SLOT), P(SLOT, None, "dp"), P(SLOT, "dp", None)),
        out_specs=P("dp", SLOT, None),
        check_vma=False,
    )
```

```python
import functools

import jax
import jax.numpy as jnp
from jax import lax
from jax.experimental import pallas as pl
from jax.experimental.pallas import tpu as pltpu
from jax.sharding import Mesh
from jax.sharding import PartitionSpec as P


X, Z, Y = "slot_0", "slot_1", "slot_2"
SLOT = (X, Z, Y)
TILE = tuple(
    tuple(((r + 2 * y) % 4 * 4 + z) * 2 + y for y in (0, 1) for z in range(4)) for r in range(4)
)
PARTNER = tuple(
    ((x * 4 + z) * 2 + y, ((x + 2) % 4 * 4 + z) * 2 + 1 - y)
    for x in range(4)
    for z in range(4)
    for y in (0, 1)
)
LANES = 128
ROOM = 24 * 1024 * 1024
VMEM = pl.BlockSpec(memory_space=pltpu.VMEM)
ANY = pl.BlockSpec(memory_space=pl.ANY)


def place(step):
    y, z = lax.axis_index(Y), lax.axis_index(Z)
    return ((y + step % 2) % 2) * 4 + (z + step // 2) % 4


def ahead(array, axis, step):
    size = lax.axis_size(axis)
    return lax.ppermute(array, axis, [((i + step) % size, i) for i in range(size)])


def swapped(array, axis, mask):
    size = lax.axis_size(axis)
    return lax.ppermute(array, axis, [(i, i ^ mask) for i in range(size)])


def all_to_all(array):
    return lax.all_to_all(
        array, SLOT, split_axis=0, concat_axis=0, axis_index_groups=TILE, tiled=True
    )


def dispatch_kernel(first, k0, k1, k2, k3, *refs):
    *blocks, message, logits, s0, s1, s2, s3, first_here, field, arrivals, loaded = refs
    owners, _, own_slots, _ = message.shape
    slots = owners * own_slots
    features = k0.shape[1]
    columns = jnp.concatenate([k0[...], k1[...], k2[...], k3[...]], axis=0)
    images, positions, _ = blocks[0].shape

    def copies(b):
        return [
            pltpu.make_async_copy(
                block.at[b], field.at[b, k * positions : (k + 1) * positions], arrivals.at[b, k]
            )
            for k, block in enumerate(blocks)
        ]

    for b in range(images):
        for copy in copies(b):
            copy.start()
    load = pltpu.make_async_copy(first, first_here, loaded)
    load.start()

    def one(b, carry):
        for copy in copies(b):
            copy.wait()
        values = lax.dot_general(
            columns,
            field[b],
            (((1,), (1,)), ((), ())),
            preferred_element_type=jnp.float32,
        )
        logits[b] = values
        row_top = jnp.max(values, axis=0, keepdims=True)
        row_total = jnp.sum(jnp.exp(values - row_top), axis=0, keepdims=True)
        row_stats = jnp.concatenate([row_top, row_total], axis=0)
        for k, out in enumerate((s0, s1, s2, s3)):
            out[b] = row_stats[:, k * positions : (k + 1) * positions]
        top = jnp.max(values, axis=1, keepdims=True).astype(jnp.bfloat16).astype(jnp.float32)
        raised = jnp.exp(values - top)
        rest = jnp.sum(raised, axis=1, keepdims=True)
        lane = lax.broadcasted_iota(jnp.int32, (slots, LANES), 1)
        stats = jnp.where(lane == 0, top, 0.0)
        for k in (1, 2, 3):
            piece = rest.astype(jnp.bfloat16).astype(jnp.float32)
            stats = jnp.where(lane == k, piece, stats)
            rest = rest - piece
        stats = stats.astype(jnp.bfloat16).reshape(owners, own_slots, LANES)
        sums = jnp.dot(
            raised.astype(jnp.bfloat16), field[b], preferred_element_type=jnp.float32
        ).astype(jnp.bfloat16)
        sums = sums.reshape(owners, own_slots, features)
        for k in range(owners):
            message[place(k), b, :, features:] = stats[k]
            message[place(k), b, :, :features] = sums[k]
        return carry

    lax.fori_loop(0, images, one, 0)
    load.wait()


def dispatch(keys, first, blocks, own_slots):
    images, positions, features = blocks[0].shape
    owners = sum(key.shape[0] for key in keys) // own_slots
    slots, width = owners * own_slots, len(blocks) * positions
    return pl.pallas_call(
        dispatch_kernel,
        out_shape=(
            jax.ShapeDtypeStruct((owners, images, own_slots, features + LANES), jnp.bfloat16),
            jax.ShapeDtypeStruct((images, slots, width), jnp.float32),
            *(jax.ShapeDtypeStruct((images, 2, positions), jnp.float32) for _ in blocks),
            jax.ShapeDtypeStruct(first.shape, first.dtype),
        ),
        in_specs=[ANY] + [VMEM] * len(keys) + [ANY] * len(blocks),
        out_specs=(VMEM,) * (3 + len(blocks)),
        scratch_shapes=[
            pltpu.VMEM((images, width, features), jnp.bfloat16),
            pltpu.SemaphoreType.DMA((images, len(blocks))),
            pltpu.SemaphoreType.DMA,
        ],
        cost_estimate=pl.CostEstimate(
            flops=4 * images * slots * width * features,
            bytes_accessed=4 * images * slots * features,
            transcendentals=2 * images * slots * width,
        ),
        compiler_params=pltpu.CompilerParams(vmem_limit_bytes=32 * 1024 * 1024),
        name="dispatch",
    )(first, *keys, *blocks)


def merge_kernel(arrived, inputs):
    owners, images, _, _ = arrived.shape
    features = inputs.shape[2]
    for b in range(images):
        tops, totals = [], []
        for k in range(owners):
            stats = arrived[k, b, :, features:].astype(jnp.float32)
            tops.append(stats[:, 0:1])
            totals.append(stats[:, 1:2] + stats[:, 2:3] + stats[:, 3:4])
        peak = functools.reduce(jnp.maximum, tops)
        scales = [jnp.exp(top - peak) for top in tops]
        whole = sum(scale * total for scale, total in zip(scales, totals))
        summed = sum(
            (scales[k] / whole) * arrived[k, b, :, :features].astype(jnp.float32)
            for k in range(owners)
        )
        inputs[b] = summed.astype(jnp.bfloat16)


def merge(arrived):
    _, images, own_slots, width = arrived.shape
    return pl.pallas_call(
        merge_kernel,
        out_shape=jax.ShapeDtypeStruct((images, own_slots, width - LANES), jnp.bfloat16),
        in_specs=[VMEM],
        out_specs=VMEM,
        cost_estimate=pl.CostEstimate(
            flops=4 * arrived.size, bytes_accessed=2 * arrived.size, transcendentals=0
        ),
        compiler_params=pltpu.CompilerParams(vmem_limit_bytes=ROOM),
        name="merge",
    )(arrived)


def expert_kernel(rows, first, second, *refs):
    *outs, second_here, loaded = refs
    rank = lax.axis_index("dp")
    experts = first.shape[0]
    images, own_slots, _ = outs[0].shape
    per_expert = own_slots // experts

    def load(expert):
        return pltpu.make_async_copy(second.at[expert], second_here.at[expert], loaded.at[expert])

    for expert in range(experts):
        load(expert).start()

    def one(expert, carry):
        cut = pl.ds(pl.multiple_of(expert * per_expert, per_expert), per_expert)
        taken = [
            rows[(rank ^ k) * images + b, cut, :]
            for k in range(len(outs))
            for b in range(images)
        ]
        hidden = jnp.dot(
            jnp.concatenate(taken, axis=0), first[expert], preferred_element_type=jnp.float32
        )
        hidden = jax.nn.gelu(hidden, approximate=True).astype(jnp.bfloat16)
        load(expert).wait()
        result = jnp.dot(hidden, second_here[expert], preferred_element_type=jnp.float32)
        for k, out in enumerate(outs):
            for b in range(images):
                at = (k * images + b) * per_expert
                out[b, cut, :] = result[at : at + per_expert].astype(out.dtype)
        return carry

    lax.fori_loop(0, experts, one, 0)


def run_experts(rows, expert_in, expert_out, ranks):
    images, own_slots = rows.shape[0] // ranks, rows.shape[1]
    shape = (images, own_slots, rows.shape[2])
    kinds = (jnp.float32, *(jnp.bfloat16 for _ in range(ranks - 1)))
    return pl.pallas_call(
        expert_kernel,
        out_shape=[jax.ShapeDtypeStruct(shape, kind) for kind in kinds],
        in_specs=[VMEM, VMEM, ANY],
        out_specs=[VMEM] * ranks,
        scratch_shapes=[
            pltpu.VMEM(expert_out.shape, expert_out.dtype),
            pltpu.SemaphoreType.DMA((expert_out.shape[0],)),
        ],
        cost_estimate=pl.CostEstimate(
            flops=4 * rows.size * expert_in.shape[2],
            bytes_accessed=4 * expert_in.size,
            transcendentals=rows.size,
        ),
        compiler_params=pltpu.CompilerParams(vmem_limit_bytes=ROOM),
        name="experts",
    )(rows, expert_in, expert_out)


def spread_kernel(own, first, second, third, copies):
    total = own[...]
    for piece in (first, second, third):
        total = total + piece[...].astype(jnp.float32)
    total = total.astype(jnp.bfloat16)
    for k in range(copies.shape[0]):
        copies[k] = total


def spread(own, pieces, count):
    return pl.pallas_call(
        spread_kernel,
        out_shape=jax.ShapeDtypeStruct((count, *own.shape), jnp.bfloat16),
        in_specs=[VMEM] * 4,
        out_specs=VMEM,
        cost_estimate=pl.CostEstimate(
            flops=4 * own.size, bytes_accessed=2 * count * own.size, transcendentals=0
        ),
        compiler_params=pltpu.CompilerParams(vmem_limit_bytes=ROOM),
        name="spread",
    )(own, *pieces)


def combine_kernel(logits, everyone, *refs):
    stats, outs = refs[:4], refs[4:]
    images, positions, _ = outs[0].shape
    owners = everyone.shape[0]

    def one(b, carry):
        outputs = jnp.concatenate([everyone[place(k), b] for k in range(owners)], axis=0)
        for r in (3, 1, 2, 0):
            values = logits[b, :, r * positions : (r + 1) * positions]
            mix = jnp.exp(values - stats[r][b][0:1]).astype(jnp.bfloat16)
            outs[r][b] = lax.dot_general(
                mix, outputs, (((0,), (0,)), ((), ())), preferred_element_type=jnp.float32
            ).astype(outs[r].dtype)
        return carry

    lax.fori_loop(0, images, one, 0)


def combine(logits, everyone, stats):
    images, slots, width = logits.shape
    shape = (images, width // len(stats), everyone.shape[3])
    kinds = (jnp.float32, jnp.bfloat16, jnp.bfloat16, jnp.bfloat16)
    return pl.pallas_call(
        combine_kernel,
        out_shape=[jax.ShapeDtypeStruct(shape, kind) for kind in kinds],
        in_specs=[VMEM] * (2 + len(stats)),
        out_specs=(VMEM,) * len(kinds),
        cost_estimate=pl.CostEstimate(
            flops=2 * images * slots * width * shape[2],
            bytes_accessed=4 * images * slots * width,
            transcendentals=images * slots * width,
        ),
        compiler_params=pltpu.CompilerParams(vmem_limit_bytes=ROOM),
        name="combine",
    )(logits, everyone, *stats)


def finish_kernel(*refs):
    parts, stats, out = refs[:4], refs[4:8], refs[8]
    images, positions, _ = out.shape
    for b in range(images):
        tops = [s[b][0:1] for s in stats]
        highest = functools.reduce(jnp.maximum, tops)
        scales = [jnp.exp(top - highest) for top in tops]
        total = sum(scale * s[b][1:2] for scale, s in zip(scales, stats))
        shares = [scale / total for scale in scales]
        shares = jnp.concatenate(shares + [jnp.zeros((LANES - 4, positions), jnp.float32)], axis=0)
        shares = shares.T
        joined = sum(
            shares[:, k : k + 1] * part[b].astype(jnp.float32) for k, part in enumerate(parts)
        )
        out[b] = joined.astype(out.dtype)


def finish(parts, stats):
    shape = parts[0].shape
    return pl.pallas_call(
        finish_kernel,
        out_shape=jax.ShapeDtypeStruct(shape, jnp.bfloat16),
        in_specs=[VMEM] * 8,
        out_specs=VMEM,
        cost_estimate=pl.CostEstimate(
            flops=8 * parts[0].size, bytes_accessed=12 * parts[0].size, transcendentals=0
        ),
        compiler_params=pltpu.CompilerParams(vmem_limit_bytes=ROOM),
        name="finish",
    )(*parts, *stats)


def shards(tokens, slot_keys, expert_in, expert_out):
    ranks = lax.axis_size("dp")
    owners = len(TILE[0])
    pair = lax.ppermute(slot_keys.T, SLOT, PARTNER)
    near = [ahead(tokens, X, 1), ahead(tokens, X, 3), ahead(tokens, Y, 1)]
    pair = jnp.concatenate([slot_keys.T, pair], axis=0)
    keys = [pair, *(ahead(pair, Z, k) for k in (1, 2, 3))]
    message, logits, *stats, first = dispatch(
        keys, expert_in, [tokens, *near], slot_keys.shape[1]
    )
    arrived = all_to_all(message)
    rows = lax.all_gather(merge(arrived), "dp", axis=0, tiled=True)
    own, *pieces = run_experts(rows, first, expert_out, ranks)
    pieces = [swapped(piece, "dp", k) for k, piece in zip((1, 2, 3), pieces)]
    back = [ahead(stats[1], X, 3), ahead(stats[2], X, 1), ahead(stats[3], Y, 1)]
    pieces, back = lax.optimization_barrier((pieces, back))
    everyone = all_to_all(spread(own, pieces, owners))
    own, right, left, up = combine(logits, everyone, stats)
    parts = [own, ahead(right, X, 3), ahead(left, X, 1), ahead(up, Y, 1)]
    return finish(parts, [stats[0], *back])


def solution(mesh):
    split = Mesh(mesh.devices.reshape(4, 4, 2, mesh.shape["dp"]), (X, Z, Y, "dp"))
    return jax.shard_map(
        shards,
        mesh=split,
        in_specs=(P("dp", SLOT, None), P(None, SLOT), P(SLOT, None, "dp"), P(SLOT, "dp", None)),
        out_specs=P("dp", SLOT, None),
        check_vma=False,
    )
```

```python
import functools

import jax
import jax.numpy as jnp
from jax import lax
from jax.experimental import pallas as pl
from jax.experimental.pallas import tpu as pltpu
from jax.sharding import Mesh
from jax.sharding import PartitionSpec as P


X, Z, Y = "slot_0", "slot_1", "slot_2"
SLOT = (X, Z, Y)
TILE = tuple(
    tuple(((r + 2 * y) % 4 * 4 + z) * 2 + y for y in (0, 1) for z in range(4)) for r in range(4)
)
PARTNER = tuple(
    ((x * 4 + z) * 2 + y, ((x + 2) % 4 * 4 + z) * 2 + 1 - y)
    for x in range(4)
    for z in range(4)
    for y in (0, 1)
)
LANES = 128
ROOM = 24 * 1024 * 1024
VMEM = pl.BlockSpec(memory_space=pltpu.VMEM)
ANY = pl.BlockSpec(memory_space=pl.ANY)
HBM = pl.BlockSpec(memory_space=pltpu.HBM)


def place(step):
    y, z = lax.axis_index(Y), lax.axis_index(Z)
    return ((y + step % 2) % 2) * 4 + (z + step // 2) % 4


def ahead(array, axis, step):
    size = lax.axis_size(axis)
    return lax.ppermute(array, axis, [((i + step) % size, i) for i in range(size)])


def swapped(array, axis, mask):
    size = lax.axis_size(axis)
    return lax.ppermute(array, axis, [(i, i ^ mask) for i in range(size)])


def all_to_all(array):
    return lax.all_to_all(
        array, SLOT, split_axis=0, concat_axis=0, axis_index_groups=TILE, tiled=True
    )


def dispatch_kernel(first, k0, k1, k2, k3, *refs):
    *blocks, message, logits, s0, s1, s2, s3, first_here, field, arrivals, loaded = refs
    owners = message.shape[0]
    slots, features = 4 * k0.shape[0], k0.shape[1]
    own_slots, tiles = slots // owners, features // LANES
    columns = jnp.concatenate([k0[...], k1[...], k2[...], k3[...]], axis=0)
    images, positions, _ = blocks[0].shape

    def copies(b):
        return [
            pltpu.make_async_copy(
                block.at[b], field.at[b, k * positions : (k + 1) * positions], arrivals.at[b, k]
            )
            for k, block in enumerate(blocks)
        ]

    for b in range(images):
        for copy in copies(b):
            copy.start()
    load = pltpu.make_async_copy(first, first_here, loaded)
    load.start()

    def one(b, carry):
        for copy in copies(b):
            copy.wait()
        values = lax.dot_general(
            columns,
            field[b],
            (((1,), (1,)), ((), ())),
            preferred_element_type=jnp.float32,
        )
        logits[b] = values
        row_top = jnp.max(values, axis=0, keepdims=True)
        row_total = jnp.sum(jnp.exp(values - row_top), axis=0, keepdims=True)
        row_stats = jnp.concatenate([row_top, row_total], axis=0)
        for k, out in enumerate((s0, s1, s2, s3)):
            out[b] = row_stats[:, k * positions : (k + 1) * positions]
        top = jnp.max(values, axis=1, keepdims=True).astype(jnp.bfloat16).astype(jnp.float32)
        raised = jnp.exp(values - top)
        rest = jnp.sum(raised, axis=1, keepdims=True)
        lane = lax.broadcasted_iota(jnp.int32, (slots, LANES), 1)
        stats = jnp.where(lane == 0, top, 0.0)
        for k in (1, 2, 3):
            piece = rest.astype(jnp.bfloat16).astype(jnp.float32)
            stats = jnp.where(lane == k, piece, stats)
            rest = rest - piece
        stats = stats.T[:8]
        sums = jnp.dot(
            raised.astype(jnp.bfloat16), field[b], preferred_element_type=jnp.float32
        ).astype(jnp.bfloat16)
        for k in range(owners):
            at, rows = place(k), slice(k * own_slots, (k + 1) * own_slots)
            for t in range(tiles):
                lanes = slice(t * LANES, (t + 1) * LANES)
                to = pl.ds(pl.multiple_of((b * tiles + t) * own_slots, own_slots), own_slots)
                message[at, to, :] = sums[rows, lanes]
            line = stats
            if k > 0:
                line = jnp.concatenate([line[:, k * own_slots :], line[:, : k * own_slots]], axis=1)
            to = pl.ds(pl.multiple_of((images * tiles) * own_slots + 8 * b, 8), 8)
            message[at, to, :] = line[:, :LANES].astype(jnp.bfloat16)
        return carry

    lax.fori_loop(0, images, one, 0)
    load.wait()


def dispatch(keys, first, blocks, own_slots):
    images, positions, features = blocks[0].shape
    owners = sum(key.shape[0] for key in keys) // own_slots
    slots, width = owners * own_slots, len(blocks) * positions
    return pl.pallas_call(
        dispatch_kernel,
        out_shape=(
            jax.ShapeDtypeStruct(
                (owners, images * (features // LANES * own_slots + 8), LANES), jnp.bfloat16
            ),
            jax.ShapeDtypeStruct((images, slots, width), jnp.float32),
            *(jax.ShapeDtypeStruct((images, 2, positions), jnp.float32) for _ in blocks),
            jax.ShapeDtypeStruct(first.shape, first.dtype),
        ),
        in_specs=[HBM] + [VMEM] * len(keys) + [HBM] + [ANY] * (len(blocks) - 1),
        out_specs=(VMEM,) * (3 + len(blocks)),
        scratch_shapes=[
            pltpu.VMEM((images, width, features), jnp.bfloat16),
            pltpu.SemaphoreType.DMA((images, len(blocks))),
            pltpu.SemaphoreType.DMA,
        ],
        cost_estimate=pl.CostEstimate(
            flops=4 * images * slots * width * features,
            bytes_accessed=4 * images * slots * features,
            transcendentals=2 * images * slots * width,
        ),
        compiler_params=pltpu.CompilerParams(vmem_limit_bytes=32 * 1024 * 1024),
        name="dispatch",
    )(first, *keys, *blocks)


def merge_kernel(arrived, inputs):
    owners = arrived.shape[0]
    images, own_slots, features = inputs.shape
    tiles = features // LANES
    for b in range(images):
        tops, totals = [], []
        for k in range(owners):
            at = images * tiles * own_slots + 8 * b
            stats = arrived[k, at : at + 8, :].astype(jnp.float32)
            tops.append(stats[0:1])
            totals.append(stats[1:2] + stats[2:3] + stats[3:4])
        peak = functools.reduce(jnp.maximum, tops)
        scales = [jnp.exp(top - peak) for top in tops]
        whole = sum(scale * total for scale, total in zip(scales, totals))
        shares = [scale / whole for scale in scales]
        shares = jnp.concatenate(
            shares + [jnp.zeros((LANES - owners, LANES), jnp.float32)], axis=0
        ).T
        for t in range(tiles):
            at = (b * tiles + t) * own_slots
            summed = sum(
                shares[:own_slots, k : k + 1]
                * arrived[k, at : at + own_slots, :].astype(jnp.float32)
                for k in range(owners)
            )
            inputs[b, :, t * LANES : (t + 1) * LANES] = summed.astype(jnp.bfloat16)


def merge(arrived, shape):
    return pl.pallas_call(
        merge_kernel,
        out_shape=jax.ShapeDtypeStruct(shape, jnp.bfloat16),
        in_specs=[VMEM],
        out_specs=VMEM,
        cost_estimate=pl.CostEstimate(
            flops=4 * arrived.size, bytes_accessed=2 * arrived.size, transcendentals=0
        ),
        compiler_params=pltpu.CompilerParams(vmem_limit_bytes=ROOM),
        name="merge",
    )(arrived)


def expert_kernel(rows, first, second, *outs):
    rank = lax.axis_index("dp")
    experts = first.shape[0]
    images, own_slots, _ = outs[0].shape
    per_expert = own_slots // experts

    def one(expert, carry):
        cut = pl.ds(pl.multiple_of(expert * per_expert, per_expert), per_expert)
        taken = [
            rows[(rank ^ k) * images + b, cut, :]
            for k in range(len(outs))
            for b in range(images)
        ]
        hidden = jnp.dot(
            jnp.concatenate(taken, axis=0), first[expert], preferred_element_type=jnp.float32
        )
        hidden = jax.nn.gelu(hidden, approximate=True).astype(jnp.bfloat16)
        result = jnp.dot(hidden, second[expert], preferred_element_type=jnp.float32)
        for k, out in enumerate(outs):
            for b in range(images):
                at = (k * images + b) * per_expert
                out[b, cut, :] = result[at : at + per_expert].astype(out.dtype)
        return carry

    lax.fori_loop(0, experts, one, 0)


def run_experts(rows, expert_in, expert_out, ranks):
    images, own_slots = rows.shape[0] // ranks, rows.shape[1]
    shape = (images, own_slots, rows.shape[2])
    kinds = (jnp.float32, *(jnp.bfloat16 for _ in range(ranks - 1)))
    return pl.pallas_call(
        expert_kernel,
        out_shape=[jax.ShapeDtypeStruct(shape, kind) for kind in kinds],
        in_specs=[VMEM] * 3,
        out_specs=[VMEM] * ranks,
        cost_estimate=pl.CostEstimate(
            flops=4 * rows.size * expert_in.shape[2],
            bytes_accessed=4 * expert_in.size,
            transcendentals=rows.size,
        ),
        compiler_params=pltpu.CompilerParams(vmem_limit_bytes=ROOM),
        name="experts",
    )(rows, expert_in, expert_out)


def spread_kernel(own, first, second, third, copies):
    total = own[...]
    for piece in (first, second, third):
        total = total + piece[...].astype(jnp.float32)
    total = total.astype(jnp.bfloat16)
    for k in range(copies.shape[0]):
        copies[k] = total


def spread(own, pieces, count):
    return pl.pallas_call(
        spread_kernel,
        out_shape=jax.ShapeDtypeStruct((count, *own.shape), jnp.bfloat16),
        in_specs=[VMEM] * 4,
        out_specs=VMEM,
        cost_estimate=pl.CostEstimate(
            flops=4 * own.size, bytes_accessed=2 * count * own.size, transcendentals=0
        ),
        compiler_params=pltpu.CompilerParams(vmem_limit_bytes=ROOM),
        name="spread",
    )(own, *pieces)


def combine_kernel(logits, everyone, *refs):
    stats, outs = refs[:4], refs[4:]
    images, positions, _ = outs[0].shape
    owners = everyone.shape[0]

    def one(b, carry):
        outputs = jnp.concatenate([everyone[place(k), b] for k in range(owners)], axis=0)
        for r in (3, 1, 2, 0):
            values = logits[b, :, r * positions : (r + 1) * positions]
            mix = jnp.exp(values - stats[r][b][0:1]).astype(jnp.bfloat16)
            outs[r][b] = lax.dot_general(
                mix, outputs, (((0,), (0,)), ((), ())), preferred_element_type=jnp.float32
            ).astype(outs[r].dtype)
        return carry

    lax.fori_loop(0, images, one, 0)


def combine(logits, everyone, stats):
    images, slots, width = logits.shape
    shape = (images, width // len(stats), everyone.shape[3])
    kinds = (jnp.float32, jnp.bfloat16, jnp.bfloat16, jnp.bfloat16)
    return pl.pallas_call(
        combine_kernel,
        out_shape=[jax.ShapeDtypeStruct(shape, kind) for kind in kinds],
        in_specs=[VMEM] * (2 + len(stats)),
        out_specs=(VMEM,) * len(kinds),
        cost_estimate=pl.CostEstimate(
            flops=2 * images * slots * width * shape[2],
            bytes_accessed=4 * images * slots * width,
            transcendentals=images * slots * width,
        ),
        compiler_params=pltpu.CompilerParams(vmem_limit_bytes=ROOM),
        name="combine",
    )(logits, everyone, *stats)


def finish_kernel(*refs):
    parts, stats, (out, ready, sent) = refs[:4], refs[4:8], refs[8:]
    images, positions, _ = out.shape
    copies = [pltpu.make_async_copy(ready.at[b], out.at[b], sent.at[b]) for b in range(images)]
    for b in range(images):
        tops = [s[b][0:1] for s in stats]
        highest = functools.reduce(jnp.maximum, tops)
        scales = [jnp.exp(top - highest) for top in tops]
        total = sum(scale * s[b][1:2] for scale, s in zip(scales, stats))
        shares = [scale / total for scale in scales]
        shares = jnp.concatenate(shares + [jnp.zeros((LANES - 4, positions), jnp.float32)], axis=0)
        shares = shares.T
        joined = sum(
            shares[:, k : k + 1] * part[b].astype(jnp.float32) for k, part in enumerate(parts)
        )
        ready[b] = joined.astype(out.dtype)
        copies[b].start()
    for copy in copies:
        copy.wait()


def finish(parts, stats):
    shape = parts[0].shape
    return pl.pallas_call(
        finish_kernel,
        out_shape=jax.ShapeDtypeStruct(shape, jnp.bfloat16),
        in_specs=[VMEM] * 8,
        out_specs=ANY,
        scratch_shapes=[
            pltpu.VMEM(shape, jnp.bfloat16),
            pltpu.SemaphoreType.DMA((shape[0],)),
        ],
        cost_estimate=pl.CostEstimate(
            flops=8 * parts[0].size, bytes_accessed=12 * parts[0].size, transcendentals=0
        ),
        compiler_params=pltpu.CompilerParams(vmem_limit_bytes=ROOM),
        name="finish",
    )(*parts, *stats)


def shards(tokens, slot_keys, expert_in, expert_out):
    ranks = lax.axis_size("dp")
    owners = len(TILE[0])
    pair = lax.ppermute(slot_keys.T, SLOT, PARTNER)
    near = [ahead(tokens, X, 1), ahead(tokens, X, 3), ahead(tokens, Y, 1)]
    pair = jnp.concatenate([slot_keys.T, pair], axis=0)
    keys = [pair, *(ahead(pair, Z, k) for k in (1, 2, 3))]
    message, logits, *stats, first = dispatch(
        keys, expert_in, [tokens, *near], slot_keys.shape[1]
    )
    arrived = all_to_all(message)
    slot_inputs = merge(arrived, (tokens.shape[0], *slot_keys.shape[::-1]))
    rows = lax.all_gather(slot_inputs, "dp", axis=0, tiled=True)
    own, *pieces = run_experts(rows, first, expert_out, ranks)
    pieces = [swapped(piece, "dp", k) for k, piece in zip((1, 2, 3), pieces)]
    back = [ahead(stats[1], X, 3), ahead(stats[2], X, 1), ahead(stats[3], Y, 1)]
    pieces, back = lax.optimization_barrier((pieces, back))
    everyone = all_to_all(spread(own, pieces, owners))
    own, right, left, up = combine(logits, everyone, stats)
    parts = [own, ahead(right, X, 3), ahead(left, X, 1), ahead(up, Y, 1)]
    return finish(parts, [stats[0], *back])


def solution(mesh):
    split = Mesh(mesh.devices.reshape(4, 4, 2, mesh.shape["dp"]), (X, Z, Y, "dp"))
    return jax.shard_map(
        shards,
        mesh=split,
        in_specs=(P("dp", SLOT, None), P(None, SLOT), P(SLOT, None, "dp"), P(SLOT, "dp", None)),
        out_specs=P("dp", SLOT, None),
        check_vma=False,
    )
```

```python
import functools

import jax
import jax.numpy as jnp
from jax import lax
from jax.experimental import pallas as pl
from jax.experimental.pallas import tpu as pltpu
from jax.sharding import Mesh
from jax.sharding import PartitionSpec as P


X, Z, Y = "slot_0", "slot_1", "slot_2"
SLOT = (X, Z, Y)
TILE = tuple(
    tuple(((r + 2 * y) % 4 * 4 + z) * 2 + y for y in (0, 1) for z in range(4)) for r in range(4)
)
PARTNER = tuple(
    ((x * 4 + z) * 2 + y, ((x + 2) % 4 * 4 + z) * 2 + 1 - y)
    for x in range(4)
    for z in range(4)
    for y in (0, 1)
)
LANES = 128
ROOM = 24 * 1024 * 1024
VMEM = pl.BlockSpec(memory_space=pltpu.VMEM)
ANY = pl.BlockSpec(memory_space=pl.ANY)
HBM = pl.BlockSpec(memory_space=pltpu.HBM)


def place(step):
    y, z = lax.axis_index(Y), lax.axis_index(Z)
    return ((y + step % 2) % 2) * 4 + (z + step // 2) % 4


def ahead(array, axis, step):
    size = lax.axis_size(axis)
    return lax.ppermute(array, axis, [((i + step) % size, i) for i in range(size)])


def swapped(array, axis, mask):
    size = lax.axis_size(axis)
    return lax.ppermute(array, axis, [(i, i ^ mask) for i in range(size)])


def all_to_all(array):
    return lax.all_to_all(
        array, SLOT, split_axis=0, concat_axis=0, axis_index_groups=TILE, tiled=True
    )


def early_kernel(first, own, k0, k1, k2, k3, first_here, own_here, logits, loaded):
    images = own.shape[0]
    columns = jnp.concatenate([k0[...], k1[...], k2[...], k3[...]], axis=0)
    blocks = [pltpu.make_async_copy(own.at[b], own_here.at[b], loaded.at[b]) for b in range(images)]
    load = pltpu.make_async_copy(first, first_here, loaded.at[images])
    for block in blocks:
        block.start()
    load.start()
    for b in range(images):
        blocks[b].wait()
        logits[b] = lax.dot_general(
            columns,
            own_here[b],
            (((1,), (1,)), ((), ())),
            preferred_element_type=jnp.float32,
        )
    load.wait()


def early(first, own, keys):
    images, positions, _ = own.shape
    slots = sum(key.shape[0] for key in keys)
    return pl.pallas_call(
        early_kernel,
        out_shape=(
            jax.ShapeDtypeStruct(first.shape, first.dtype),
            jax.ShapeDtypeStruct(own.shape, own.dtype),
            jax.ShapeDtypeStruct((images, slots, positions), jnp.float32),
        ),
        in_specs=[HBM] * 2 + [VMEM] * len(keys),
        out_specs=(VMEM,) * 3,
        scratch_shapes=[pltpu.SemaphoreType.DMA((images + 1,))],
        cost_estimate=pl.CostEstimate(
            flops=2 * slots * own.size, bytes_accessed=2 * first.size, transcendentals=0
        ),
        compiler_params=pltpu.CompilerParams(vmem_limit_bytes=40 * 1024 * 1024),
        name="early",
    )(first, own, *keys)


def dispatch_kernel(own_logits, k0, k1, k2, k3, *refs):
    *blocks, message, logits, s0, s1, s2, s3, field, arrivals = refs
    owners = message.shape[0]
    slots, features = 4 * k0.shape[0], k0.shape[1]
    own_slots, tiles = slots // owners, features // LANES
    columns = jnp.concatenate([k0[...], k1[...], k2[...], k3[...]], axis=0)
    images, positions, _ = blocks[0].shape

    def copies(b):
        return [
            pltpu.make_async_copy(
                block.at[b], field.at[b, k * positions : (k + 1) * positions], arrivals.at[b, k]
            )
            for k, block in enumerate(blocks)
        ]

    for b in range(images):
        for copy in copies(b):
            copy.start()

    def one(b, carry):
        for copy in copies(b):
            copy.wait()
        near = lax.dot_general(
            columns,
            field[b, positions:],
            (((1,), (1,)), ((), ())),
            preferred_element_type=jnp.float32,
        )
        values = jnp.concatenate([own_logits[b], near], axis=1)
        logits[b] = values
        row_top = jnp.max(values, axis=0, keepdims=True)
        row_total = jnp.sum(jnp.exp(values - row_top), axis=0, keepdims=True)
        row_stats = jnp.concatenate([row_top, row_total], axis=0)
        for k, out in enumerate((s0, s1, s2, s3)):
            out[b] = row_stats[:, k * positions : (k + 1) * positions]
        top = jnp.max(values, axis=1, keepdims=True).astype(jnp.bfloat16).astype(jnp.float32)
        raised = jnp.exp(values - top)
        rest = jnp.sum(raised, axis=1, keepdims=True)
        lane = lax.broadcasted_iota(jnp.int32, (slots, LANES), 1)
        stats = jnp.where(lane == 0, top, 0.0)
        for k in (1, 2, 3):
            piece = rest.astype(jnp.bfloat16).astype(jnp.float32)
            stats = jnp.where(lane == k, piece, stats)
            rest = rest - piece
        stats = stats.T[:8]
        sums = jnp.dot(
            raised.astype(jnp.bfloat16), field[b], preferred_element_type=jnp.float32
        ).astype(jnp.bfloat16)
        for k in range(owners):
            at, rows = place(k), slice(k * own_slots, (k + 1) * own_slots)
            for t in range(tiles):
                lanes = slice(t * LANES, (t + 1) * LANES)
                to = pl.ds(pl.multiple_of((b * tiles + t) * own_slots, own_slots), own_slots)
                message[at, to, :] = sums[rows, lanes]
            line = stats
            if k > 0:
                line = jnp.concatenate([line[:, k * own_slots :], line[:, : k * own_slots]], axis=1)
            to = pl.ds(pl.multiple_of((images * tiles) * own_slots + 8 * b, 8), 8)
            message[at, to, :] = line[:, :LANES].astype(jnp.bfloat16)
        return carry

    lax.fori_loop(0, images, one, 0)


def dispatch(own_logits, keys, blocks, own_slots):
    images, positions, features = blocks[0].shape
    owners = sum(key.shape[0] for key in keys) // own_slots
    slots, width = owners * own_slots, len(blocks) * positions
    return pl.pallas_call(
        dispatch_kernel,
        out_shape=(
            jax.ShapeDtypeStruct(
                (owners, images * (features // LANES * own_slots + 8), LANES), jnp.bfloat16
            ),
            jax.ShapeDtypeStruct((images, slots, width), jnp.float32),
            *(jax.ShapeDtypeStruct((images, 2, positions), jnp.float32) for _ in blocks),
        ),
        in_specs=[VMEM] + [VMEM] * len(keys) + [ANY] * len(blocks),
        out_specs=(VMEM,) * (2 + len(blocks)),
        scratch_shapes=[
            pltpu.VMEM((images, width, features), jnp.bfloat16),
            pltpu.SemaphoreType.DMA((images, len(blocks))),
        ],
        cost_estimate=pl.CostEstimate(
            flops=4 * images * slots * width * features,
            bytes_accessed=4 * images * slots * features,
            transcendentals=2 * images * slots * width,
        ),
        compiler_params=pltpu.CompilerParams(vmem_limit_bytes=32 * 1024 * 1024),
        name="dispatch",
    )(own_logits, *keys, *blocks)


def merge_kernel(arrived, inputs):
    owners = arrived.shape[0]
    images, own_slots, features = inputs.shape
    tiles = features // LANES
    for b in range(images):
        tops, totals = [], []
        for k in range(owners):
            at = images * tiles * own_slots + 8 * b
            stats = arrived[k, at : at + 8, :].astype(jnp.float32)
            tops.append(stats[0:1])
            totals.append(stats[1:2] + stats[2:3] + stats[3:4])
        peak = functools.reduce(jnp.maximum, tops)
        scales = [jnp.exp(top - peak) for top in tops]
        whole = sum(scale * total for scale, total in zip(scales, totals))
        shares = [scale / whole for scale in scales]
        shares = jnp.concatenate(
            shares + [jnp.zeros((LANES - owners, LANES), jnp.float32)], axis=0
        ).T
        for t in range(tiles):
            at = (b * tiles + t) * own_slots
            summed = sum(
                shares[:own_slots, k : k + 1]
                * arrived[k, at : at + own_slots, :].astype(jnp.float32)
                for k in range(owners)
            )
            inputs[b, :, t * LANES : (t + 1) * LANES] = summed.astype(jnp.bfloat16)


def merge(arrived, shape):
    return pl.pallas_call(
        merge_kernel,
        out_shape=jax.ShapeDtypeStruct(shape, jnp.bfloat16),
        in_specs=[VMEM],
        out_specs=VMEM,
        cost_estimate=pl.CostEstimate(
            flops=4 * arrived.size, bytes_accessed=2 * arrived.size, transcendentals=0
        ),
        compiler_params=pltpu.CompilerParams(vmem_limit_bytes=ROOM),
        name="merge",
    )(arrived)


def expert_kernel(rows, first, second, *outs):
    rank = lax.axis_index("dp")
    experts = first.shape[0]
    images, own_slots, _ = outs[0].shape
    per_expert = own_slots // experts

    def one(expert, carry):
        cut = pl.ds(pl.multiple_of(expert * per_expert, per_expert), per_expert)
        taken = [
            rows[(rank ^ k) * images + b, cut, :]
            for k in range(len(outs))
            for b in range(images)
        ]
        hidden = jnp.dot(
            jnp.concatenate(taken, axis=0), first[expert], preferred_element_type=jnp.float32
        )
        hidden = jax.nn.gelu(hidden, approximate=True).astype(jnp.bfloat16)
        result = jnp.dot(hidden, second[expert], preferred_element_type=jnp.float32)
        for k, out in enumerate(outs):
            for b in range(images):
                at = (k * images + b) * per_expert
                out[b, cut, :] = result[at : at + per_expert].astype(out.dtype)
        return carry

    lax.fori_loop(0, experts, one, 0)


def run_experts(rows, expert_in, expert_out, ranks):
    images, own_slots = rows.shape[0] // ranks, rows.shape[1]
    shape = (images, own_slots, rows.shape[2])
    kinds = (jnp.float32, *(jnp.bfloat16 for _ in range(ranks - 1)))
    return pl.pallas_call(
        expert_kernel,
        out_shape=[jax.ShapeDtypeStruct(shape, kind) for kind in kinds],
        in_specs=[VMEM] * 3,
        out_specs=[VMEM] * ranks,
        cost_estimate=pl.CostEstimate(
            flops=4 * rows.size * expert_in.shape[2],
            bytes_accessed=4 * expert_in.size,
            transcendentals=rows.size,
        ),
        compiler_params=pltpu.CompilerParams(vmem_limit_bytes=ROOM),
        name="experts",
    )(rows, expert_in, expert_out)


def spread_kernel(own, first, second, third, copies):
    total = own[...]
    for piece in (first, second, third):
        total = total + piece[...].astype(jnp.float32)
    total = total.astype(jnp.bfloat16)
    for k in range(copies.shape[0]):
        copies[k] = total


def spread(own, pieces, count):
    return pl.pallas_call(
        spread_kernel,
        out_shape=jax.ShapeDtypeStruct((count, *own.shape), jnp.bfloat16),
        in_specs=[VMEM] * 4,
        out_specs=VMEM,
        cost_estimate=pl.CostEstimate(
            flops=4 * own.size, bytes_accessed=2 * count * own.size, transcendentals=0
        ),
        compiler_params=pltpu.CompilerParams(vmem_limit_bytes=ROOM),
        name="spread",
    )(own, *pieces)


def combine_kernel(blocks, logits, everyone, *refs):
    stats, outs = refs[: len(blocks)], refs[len(blocks) :]
    images, positions, _ = outs[0].shape
    owners = everyone.shape[0]

    def one(b, carry):
        outputs = jnp.concatenate([everyone[place(k), b] for k in range(owners)], axis=0)
        for block, stat, out in zip(blocks, stats, outs):
            values = logits[b, :, block * positions : (block + 1) * positions]
            mix = jnp.exp(values - stat[b][0:1]).astype(jnp.bfloat16)
            out[b] = lax.dot_general(
                mix, outputs, (((0,), (0,)), ((), ())), preferred_element_type=jnp.float32
            ).astype(out.dtype)
        return carry

    lax.fori_loop(0, images, one, 0)


def combine(blocks, kind, logits, everyone, stats):
    images, slots, _ = logits.shape
    shape = (images, stats[0].shape[2], everyone.shape[3])
    return pl.pallas_call(
        functools.partial(combine_kernel, blocks),
        out_shape=[jax.ShapeDtypeStruct(shape, kind) for _ in blocks],
        in_specs=[VMEM] * (2 + len(blocks)),
        out_specs=[VMEM] * len(blocks),
        cost_estimate=pl.CostEstimate(
            flops=2 * len(blocks) * slots * images * shape[1] * shape[2],
            bytes_accessed=4 * logits.size,
            transcendentals=logits.size,
        ),
        compiler_params=pltpu.CompilerParams(vmem_limit_bytes=ROOM),
        name="combine",
    )(logits, everyone, *(stats[block] for block in blocks))


def finish_kernel(*refs):
    parts, stats, (out, ready, sent) = refs[:4], refs[4:8], refs[8:]
    images, positions, _ = out.shape
    copies = [pltpu.make_async_copy(ready.at[b], out.at[b], sent.at[b]) for b in range(images)]
    for b in range(images):
        tops = [s[b][0:1] for s in stats]
        highest = functools.reduce(jnp.maximum, tops)
        scales = [jnp.exp(top - highest) for top in tops]
        total = sum(scale * s[b][1:2] for scale, s in zip(scales, stats))
        shares = [scale / total for scale in scales]
        shares = jnp.concatenate(shares + [jnp.zeros((LANES - 4, positions), jnp.float32)], axis=0)
        shares = shares.T
        for t in range(out.shape[2] // LANES):
            lanes = slice(t * LANES, (t + 1) * LANES)
            joined = sum(
                shares[:, k : k + 1] * part[b, :, lanes].astype(jnp.float32)
                for k, part in enumerate(parts)
            )
            ready[b, :, lanes] = joined.astype(out.dtype)
        copies[b].start()
    for copy in copies:
        copy.wait()


def finish(parts, stats):
    shape = parts[0].shape
    return pl.pallas_call(
        finish_kernel,
        out_shape=jax.ShapeDtypeStruct(shape, jnp.bfloat16),
        in_specs=[VMEM] * 8,
        out_specs=ANY,
        scratch_shapes=[
            pltpu.VMEM(shape, jnp.bfloat16),
            pltpu.SemaphoreType.DMA((shape[0],)),
        ],
        cost_estimate=pl.CostEstimate(
            flops=8 * parts[0].size, bytes_accessed=12 * parts[0].size, transcendentals=0
        ),
        compiler_params=pltpu.CompilerParams(vmem_limit_bytes=ROOM),
        name="finish",
    )(*parts, *stats)


def shards(tokens, slot_keys, expert_in, expert_out):
    ranks = lax.axis_size("dp")
    owners = len(TILE[0])
    pair = lax.ppermute(slot_keys.T, SLOT, PARTNER)
    near = [ahead(tokens, X, 1), ahead(tokens, X, 3), ahead(tokens, Y, 1)]
    pair = jnp.concatenate([slot_keys.T, pair], axis=0)
    keys = [pair, *(ahead(pair, Z, k) for k in (1, 2, 3))]
    first, own, own_logits = early(expert_in, tokens, keys)
    message, logits, *stats = dispatch(own_logits, keys, [own, *near], slot_keys.shape[1])
    arrived = all_to_all(message)
    slot_inputs = merge(arrived, (tokens.shape[0], *slot_keys.shape[::-1]))
    rows = lax.all_gather(slot_inputs, "dp", axis=0, tiled=True)
    own, *pieces = run_experts(rows, first, expert_out, ranks)
    pieces = [swapped(piece, "dp", k) for k, piece in zip((1, 2, 3), pieces)]
    back = [ahead(stats[1], X, 3), ahead(stats[2], X, 1), ahead(stats[3], Y, 1)]
    pieces, back = lax.optimization_barrier((pieces, back))
    everyone = all_to_all(spread(own, pieces, owners))
    right, left, up = combine((1, 2, 3), jnp.bfloat16, logits, everyone, stats)
    parts = [ahead(right, X, 3), ahead(left, X, 1), ahead(up, Y, 1)]
    parts = [*combine((0,), jnp.float32, logits, everyone, stats), *parts]
    return finish(parts, [stats[0], *back])


def solution(mesh):
    split = Mesh(mesh.devices.reshape(4, 4, 2, mesh.shape["dp"]), (X, Z, Y, "dp"))
    return jax.shard_map(
        shards,
        mesh=split,
        in_specs=(P("dp", SLOT, None), P(None, SLOT), P(SLOT, None, "dp"), P(SLOT, "dp", None)),
        out_specs=P("dp", SLOT, None),
        check_vma=False,
    )
```

```python
import functools

import jax
import jax.numpy as jnp
from jax import lax
from jax.experimental import pallas as pl
from jax.experimental.pallas import tpu as pltpu
from jax.sharding import Mesh
from jax.sharding import PartitionSpec as P


X, Z, Y = "slot_0", "slot_1", "slot_2"
SLOT = (X, Z, Y)
TILE = tuple(
    tuple(((r + 2 * y) % 4 * 4 + z) * 2 + y for y in (0, 1) for z in range(4)) for r in range(4)
)
PARTNER = tuple(
    ((x * 4 + z) * 2 + y, ((x + 2) % 4 * 4 + z) * 2 + 1 - y)
    for x in range(4)
    for z in range(4)
    for y in (0, 1)
)
LANES = 128
ROOM = 24 * 1024 * 1024
VMEM = pl.BlockSpec(memory_space=pltpu.VMEM)
ANY = pl.BlockSpec(memory_space=pl.ANY)
HBM = pl.BlockSpec(memory_space=pltpu.HBM)


def place(step):
    y, z = lax.axis_index(Y), lax.axis_index(Z)
    return ((y + step % 2) % 2) * 4 + (z + step // 2) % 4


def ahead(array, axis, step):
    size = lax.axis_size(axis)
    return lax.ppermute(array, axis, [((i + step) % size, i) for i in range(size)])


def swapped(array, axis, mask):
    size = lax.axis_size(axis)
    return lax.ppermute(array, axis, [(i, i ^ mask) for i in range(size)])


def all_to_all(array):
    return lax.all_to_all(
        array, SLOT, split_axis=0, concat_axis=0, axis_index_groups=TILE, tiled=True
    )


def early_kernel(first, own, k0, k1, k2, k3, first_here, own_here, logits, loaded):
    images = own.shape[0]
    columns = jnp.concatenate([k0[...], k1[...], k2[...], k3[...]], axis=0)
    blocks = [pltpu.make_async_copy(own.at[b], own_here.at[b], loaded.at[b]) for b in range(images)]
    load = pltpu.make_async_copy(first, first_here, loaded.at[images])
    for block in blocks:
        block.start()
    load.start()
    for b in range(images):
        blocks[b].wait()
        logits[b] = lax.dot_general(
            columns,
            own_here[b],
            (((1,), (1,)), ((), ())),
            preferred_element_type=jnp.float32,
        )
    load.wait()


def early(first, own, keys):
    images, positions, _ = own.shape
    slots = sum(key.shape[0] for key in keys)
    return pl.pallas_call(
        early_kernel,
        out_shape=(
            jax.ShapeDtypeStruct(first.shape, first.dtype),
            jax.ShapeDtypeStruct(own.shape, own.dtype),
            jax.ShapeDtypeStruct((images, slots, positions), jnp.float32),
        ),
        in_specs=[HBM] * 2 + [VMEM] * len(keys),
        out_specs=(VMEM,) * 3,
        scratch_shapes=[pltpu.SemaphoreType.DMA((images + 1,))],
        cost_estimate=pl.CostEstimate(
            flops=2 * slots * own.size, bytes_accessed=2 * first.size, transcendentals=0
        ),
        compiler_params=pltpu.CompilerParams(vmem_limit_bytes=40 * 1024 * 1024),
        name="early",
    )(first, own, *keys)


def dispatch_kernel(own_logits, k0, k1, k2, k3, *refs):
    *blocks, message, logits, s0, s1, s2, s3, field, arrivals = refs
    owners = message.shape[0]
    slots, features = 4 * k0.shape[0], k0.shape[1]
    own_slots, tiles = slots // owners, features // LANES
    columns = jnp.concatenate([k0[...], k1[...], k2[...], k3[...]], axis=0)
    images, positions, _ = blocks[0].shape

    def copies(b):
        return [
            pltpu.make_async_copy(
                block.at[b], field.at[b, k * positions : (k + 1) * positions], arrivals.at[b, k]
            )
            for k, block in enumerate(blocks)
        ]

    for b in range(images):
        for copy in copies(b):
            copy.start()

    def one(b, carry):
        for copy in copies(b):
            copy.wait()
        near = lax.dot_general(
            columns,
            field[b, positions:],
            (((1,), (1,)), ((), ())),
            preferred_element_type=jnp.float32,
        )
        values = jnp.concatenate([own_logits[b], near], axis=1)
        logits[b] = values
        row_top = jnp.max(values, axis=0, keepdims=True)
        row_total = jnp.sum(jnp.exp(values - row_top), axis=0, keepdims=True)
        row_stats = jnp.concatenate([row_top, row_total], axis=0)
        for k, out in enumerate((s0, s1, s2, s3)):
            out[b] = row_stats[:, k * positions : (k + 1) * positions]
        top = jnp.max(values, axis=1, keepdims=True).astype(jnp.bfloat16).astype(jnp.float32)
        raised = jnp.exp(values - top)
        rest = jnp.sum(raised, axis=1, keepdims=True)
        lane = lax.broadcasted_iota(jnp.int32, (slots, LANES), 1)
        stats = jnp.where(lane == 0, top, 0.0)
        for k in (1, 2, 3):
            piece = rest.astype(jnp.bfloat16).astype(jnp.float32)
            stats = jnp.where(lane == k, piece, stats)
            rest = rest - piece
        stats = stats.T[:8]
        sums = jnp.dot(
            raised.astype(jnp.bfloat16), field[b], preferred_element_type=jnp.float32
        ).astype(jnp.bfloat16)
        for k in range(owners):
            at, rows = place(k), slice(k * own_slots, (k + 1) * own_slots)
            for t in range(tiles):
                lanes = slice(t * LANES, (t + 1) * LANES)
                to = pl.ds(pl.multiple_of((b * tiles + t) * own_slots, own_slots), own_slots)
                message[at, to, :] = sums[rows, lanes]
            line = stats
            if k > 0:
                line = jnp.concatenate([line[:, k * own_slots :], line[:, : k * own_slots]], axis=1)
            to = pl.ds(pl.multiple_of((images * tiles) * own_slots + 8 * b, 8), 8)
            message[at, to, :] = line[:, :LANES].astype(jnp.bfloat16)
        return carry

    lax.fori_loop(0, images, one, 0)


def dispatch(own_logits, keys, blocks, own_slots):
    images, positions, features = blocks[0].shape
    owners = sum(key.shape[0] for key in keys) // own_slots
    slots, width = owners * own_slots, len(blocks) * positions
    return pl.pallas_call(
        dispatch_kernel,
        out_shape=(
            jax.ShapeDtypeStruct(
                (owners, images * (features // LANES * own_slots + 8), LANES), jnp.bfloat16
            ),
            jax.ShapeDtypeStruct((images, slots, width), jnp.float32),
            *(jax.ShapeDtypeStruct((images, 2, positions), jnp.float32) for _ in blocks),
        ),
        in_specs=[VMEM] + [VMEM] * len(keys) + [ANY] * len(blocks),
        out_specs=(VMEM,) * (2 + len(blocks)),
        scratch_shapes=[
            pltpu.VMEM((images, width, features), jnp.bfloat16),
            pltpu.SemaphoreType.DMA((images, len(blocks))),
        ],
        cost_estimate=pl.CostEstimate(
            flops=4 * images * slots * width * features,
            bytes_accessed=4 * images * slots * features,
            transcendentals=2 * images * slots * width,
        ),
        compiler_params=pltpu.CompilerParams(vmem_limit_bytes=32 * 1024 * 1024),
        name="dispatch",
    )(own_logits, *keys, *blocks)


def merge_kernel(arrived, inputs):
    owners = arrived.shape[0]
    images, own_slots, features = inputs.shape
    tiles = features // LANES
    for b in range(images):
        tops, totals = [], []
        for k in range(owners):
            at = images * tiles * own_slots + 8 * b
            stats = arrived[k, at : at + 8, :].astype(jnp.float32)
            tops.append(stats[0:1])
            totals.append(stats[1:2] + stats[2:3] + stats[3:4])
        peak = functools.reduce(jnp.maximum, tops)
        scales = [jnp.exp(top - peak) for top in tops]
        whole = sum(scale * total for scale, total in zip(scales, totals))
        shares = [scale / whole for scale in scales]
        shares = jnp.concatenate(
            shares + [jnp.zeros((LANES - owners, LANES), jnp.float32)], axis=0
        ).T
        for t in range(tiles):
            at = (b * tiles + t) * own_slots
            summed = sum(
                shares[:own_slots, k : k + 1]
                * arrived[k, at : at + own_slots, :].astype(jnp.float32)
                for k in range(owners)
            )
            inputs[b, :, t * LANES : (t + 1) * LANES] = summed.astype(jnp.bfloat16)


def merge(arrived, shape):
    return pl.pallas_call(
        merge_kernel,
        out_shape=jax.ShapeDtypeStruct(shape, jnp.bfloat16),
        in_specs=[VMEM],
        out_specs=VMEM,
        cost_estimate=pl.CostEstimate(
            flops=4 * arrived.size, bytes_accessed=2 * arrived.size, transcendentals=0
        ),
        compiler_params=pltpu.CompilerParams(vmem_limit_bytes=ROOM),
        name="merge",
    )(arrived)


def expert_kernel(rows, first, second, *outs):
    rank = lax.axis_index("dp")
    experts = first.shape[0]
    images, own_slots, _ = outs[0].shape
    per_expert = own_slots // experts

    def one(expert, carry):
        cut = pl.ds(pl.multiple_of(expert * per_expert, per_expert), per_expert)
        taken = [
            rows[(rank ^ k) * images + b, cut, :]
            for k in range(len(outs))
            for b in range(images)
        ]
        hidden = jnp.dot(
            jnp.concatenate(taken, axis=0), first[expert], preferred_element_type=jnp.float32
        )
        hidden = jax.nn.gelu(hidden, approximate=True).astype(jnp.bfloat16)
        result = jnp.dot(hidden, second[expert], preferred_element_type=jnp.float32)
        for k, out in enumerate(outs):
            for b in range(images):
                at = (k * images + b) * per_expert
                out[b, cut, :] = result[at : at + per_expert].astype(out.dtype)
        return carry

    lax.fori_loop(0, experts, one, 0)


def run_experts(rows, expert_in, expert_out, ranks):
    images, own_slots = rows.shape[0] // ranks, rows.shape[1]
    shape = (images, own_slots, rows.shape[2])
    kinds = (jnp.float32, *(jnp.bfloat16 for _ in range(ranks - 1)))
    return pl.pallas_call(
        expert_kernel,
        out_shape=[jax.ShapeDtypeStruct(shape, kind) for kind in kinds],
        in_specs=[VMEM] * 3,
        out_specs=[VMEM] * ranks,
        cost_estimate=pl.CostEstimate(
            flops=4 * rows.size * expert_in.shape[2],
            bytes_accessed=4 * expert_in.size,
            transcendentals=rows.size,
        ),
        compiler_params=pltpu.CompilerParams(vmem_limit_bytes=ROOM),
        name="experts",
    )(rows, expert_in, expert_out)


def total_kernel(own, first, second, third, out):
    total = own[...]
    for piece in (first, second, third):
        total = total + piece[...].astype(jnp.float32)
    out[...] = total.astype(jnp.bfloat16)


def add_up(own, pieces):
    return pl.pallas_call(
        total_kernel,
        out_shape=jax.ShapeDtypeStruct(own.shape, jnp.bfloat16),
        in_specs=[VMEM] * 4,
        out_specs=VMEM,
        cost_estimate=pl.CostEstimate(
            flops=4 * own.size, bytes_accessed=12 * own.size, transcendentals=0
        ),
        compiler_params=pltpu.CompilerParams(vmem_limit_bytes=ROOM),
        name="total",
    )(own, *pieces)


def combine_kernel(blocks, logits, *refs):
    everyone, refs = refs[:8], refs[8:]
    stats, outs = refs[: len(blocks)], refs[len(blocks) :]
    images, positions, _ = outs[0].shape

    def one(b, carry):
        outputs = jnp.concatenate([piece[b] for piece in everyone], axis=0)
        for block, stat, out in zip(blocks, stats, outs):
            values = logits[b, :, block * positions : (block + 1) * positions]
            mix = jnp.exp(values - stat[b][0:1]).astype(jnp.bfloat16)
            out[b] = lax.dot_general(
                mix, outputs, (((0,), (0,)), ((), ())), preferred_element_type=jnp.float32
            ).astype(out.dtype)
        return carry

    lax.fori_loop(0, images, one, 0)


def combine(blocks, kind, logits, everyone, stats):
    images, slots, _ = logits.shape
    shape = (images, stats[0].shape[2], everyone[0].shape[2])
    return pl.pallas_call(
        functools.partial(combine_kernel, blocks),
        out_shape=[jax.ShapeDtypeStruct(shape, kind) for _ in blocks],
        in_specs=[VMEM] * (1 + len(everyone) + len(blocks)),
        out_specs=[VMEM] * len(blocks),
        cost_estimate=pl.CostEstimate(
            flops=2 * len(blocks) * slots * images * shape[1] * shape[2],
            bytes_accessed=4 * logits.size,
            transcendentals=logits.size,
        ),
        compiler_params=pltpu.CompilerParams(vmem_limit_bytes=ROOM),
        name="combine",
    )(logits, *everyone, *(stats[block] for block in blocks))


def finish_kernel(*refs):
    parts, stats, (out, ready, sent) = refs[:4], refs[4:8], refs[8:]
    images, positions, _ = out.shape
    copies = [pltpu.make_async_copy(ready.at[b], out.at[b], sent.at[b]) for b in range(images)]
    for b in range(images):
        tops = [s[b][0:1] for s in stats]
        highest = functools.reduce(jnp.maximum, tops)
        scales = [jnp.exp(top - highest) for top in tops]
        total = sum(scale * s[b][1:2] for scale, s in zip(scales, stats))
        shares = [scale / total for scale in scales]
        shares = jnp.concatenate(shares + [jnp.zeros((LANES - 4, positions), jnp.float32)], axis=0)
        shares = shares.T
        for t in range(out.shape[2] // LANES):
            lanes = slice(t * LANES, (t + 1) * LANES)
            joined = sum(
                shares[:, k : k + 1] * part[b, :, lanes].astype(jnp.float32)
                for k, part in enumerate(parts)
            )
            ready[b, :, lanes] = joined.astype(out.dtype)
        copies[b].start()
    for copy in copies:
        copy.wait()


def finish(parts, stats):
    shape = parts[0].shape
    return pl.pallas_call(
        finish_kernel,
        out_shape=jax.ShapeDtypeStruct(shape, jnp.bfloat16),
        in_specs=[VMEM] * 8,
        out_specs=ANY,
        scratch_shapes=[
            pltpu.VMEM(shape, jnp.bfloat16),
            pltpu.SemaphoreType.DMA((shape[0],)),
        ],
        cost_estimate=pl.CostEstimate(
            flops=8 * parts[0].size, bytes_accessed=12 * parts[0].size, transcendentals=0
        ),
        compiler_params=pltpu.CompilerParams(vmem_limit_bytes=ROOM),
        name="finish",
    )(*parts, *stats)


def shards(tokens, slot_keys, expert_in, expert_out):
    ranks = lax.axis_size("dp")
    pair = lax.ppermute(slot_keys.T, SLOT, PARTNER)
    near = [ahead(tokens, X, 1), ahead(tokens, X, 3), ahead(tokens, Y, 1)]
    pair = jnp.concatenate([slot_keys.T, pair], axis=0)
    keys = [pair, *(ahead(pair, Z, k) for k in (1, 2, 3))]
    first, own, own_logits = early(expert_in, tokens, keys)
    message, logits, *stats = dispatch(own_logits, keys, [own, *near], slot_keys.shape[1])
    arrived = all_to_all(message)
    slot_inputs = merge(arrived, (tokens.shape[0], *slot_keys.shape[::-1]))
    rows = lax.all_gather(slot_inputs, "dp", axis=0, tiled=True)
    own, *pieces = run_experts(rows, first, expert_out, ranks)
    pieces = [swapped(piece, "dp", k) for k, piece in zip((1, 2, 3), pieces)]
    back = [ahead(stats[1], X, 3), ahead(stats[2], X, 1), ahead(stats[3], Y, 1)]
    pieces, back = lax.optimization_barrier((pieces, back))
    here = add_up(own, pieces)
    there = lax.ppermute(here, SLOT, PARTNER)
    after, before = ahead(here, Z, 1), ahead(here, Z, 3)
    across = ahead(here, Z, 2)
    there_after, there_before = ahead(there, Z, 1), ahead(there, Z, 3)
    there_across = ahead(there_before, Z, 3)
    everyone = [here, there, after, there_after, across, there_across, before, there_before]
    right, left, up = combine((1, 2, 3), jnp.bfloat16, logits, everyone, stats)
    parts = [ahead(right, X, 3), ahead(left, X, 1), ahead(up, Y, 1)]
    parts = [*combine((0,), jnp.float32, logits, everyone, stats), *parts]
    return finish(parts, [stats[0], *back])


def solution(mesh):
    split = Mesh(mesh.devices.reshape(4, 4, 2, mesh.shape["dp"]), (X, Z, Y, "dp"))
    return jax.shard_map(
        shards,
        mesh=split,
        in_specs=(P("dp", SLOT, None), P(None, SLOT), P(SLOT, None, "dp"), P(SLOT, "dp", None)),
        out_specs=P("dp", SLOT, None),
        check_vma=False,
    )
```
